32 devices in a mesh: section: 2 (over x), dp: 16 (over z, y, core).
Axes of the slice: x: 2, y: 2, z: 4, core: 2. Of those that a mesh axis runs over, the one named last changes fastest.
Arguments:
- inputs: bfloat16 [4, 2048, 1536], P(None, 'dp'), may hold values from -6 to 6
- out_grad: bfloat16 [4, 2048, 1536], P(None, 'dp'), may hold values from -0.125 to 0.125
- guide_bin: int32 [4, 1], replicated, may hold values from 0 to 31
- time_step: int32 [4, 1], replicated, may hold values from 0 to 999
- guide_table: bfloat16 [32, 4608], replicated, may hold values from -3 to 3
- section_table: float32 [2, 3, 1536], P('section'), may hold values from -3 to 3
- value_weight: bfloat16 [2, 1536, 1536], P('section'), may hold values from -0.15625 to 0.15625
- proj_weight: bfloat16 [2, 1536, 1536], P('section'), may hold values from -0.15625 to 0.15625
Outputs:
- value_grad: float32 [2, 1536, 1536], P('section', 'dp')
- proj_grad: float32 [2, 1536, 1536], P('section', 'dp')
- table_grad: float32 [2, 3, 1536], P('section', None, 'dp')
The draws below stay inside these ranges and needn't reach their ends.
All inputs are finite; a program needn't handle non-finite values.
Results may differ from the reference program's by a relative error of at most 0.017.
Values may be sent and summed in bfloat16 or wider, within the bound.
A program may use at most 128 MiB of HBM per device.

```python
import math
import jax
import jax.numpy as jnp
from jax import lax

D = 1536
H = 1536
MICRO = 4
BINS = 32
STEPS = 1000
TOKENS = 2048
SAMPLES = 1
BLOCKS = 2


def plant(drawn, own_key, least, high):
    dims = drawn.shape
    spot = [jax.random.randint(jax.random.fold_in(own_key, axis), (), 0, dims[axis]) for axis in range(len(dims))]
    drawn = drawn.at[tuple(spot)].set(least)
    longest = dims.index(max(dims))
    spot[longest] = (spot[longest] + 1) % dims[longest]
    return drawn.at[tuple(spot)].set(high)


def levels(key, extent, cuts, least, top_value):
    def one(axis_at, blocks):
        steps = jax.random.uniform(jax.random.fold_in(jax.random.fold_in(key, 6), axis_at), (blocks,), jnp.float32, least / len(cuts), top_value / len(cuts))
        return jnp.repeat(jnp.exp(steps), extent[axis_at] // blocks).reshape((-1,) + (1,) * (len(extent) - axis_at - 1))

    factor_of = one(*cuts[0])
    for cut in cuts[1:]:
        factor_of = factor_of * one(*cut)
    return factor_of


def normal_values(stream_key, extent, deviation, bound, pieces=(), kind=jnp.bfloat16):
    array = jax.random.normal(stream_key, extent, jnp.float32) * deviation
    if len(pieces) > 0:
        array = levels(stream_key, extent, pieces, -0.22, 0.18) * array
    return jnp.clip(array, min=-bound, max=bound).astype(kind)


def setup_inputs(seed: int = 0) -> dict:
    arg_keys = jax.random.split(jax.random.key(seed), 9)
    inputs = normal_values(arg_keys[0], (MICRO, TOKENS, D), 1.0, 6.0, ((1, 16),))
    out_grad = normal_values(arg_keys[1], (MICRO, TOKENS, D), TOKENS ** -0.5, 0.125, ((1, 16),))
    guide_bin = plant(jax.random.randint(arg_keys[2], (MICRO, SAMPLES), 0, BINS), jax.random.fold_in(arg_keys[2], 1), 0, BINS - 1).astype(jnp.int32)
    time_step = plant(jax.random.randint(arg_keys[3], (MICRO, SAMPLES), 0, STEPS), jax.random.fold_in(arg_keys[3], 1), 0, STEPS - 1).astype(jnp.int32)
    guide_table = normal_values(arg_keys[4], (BINS, 3 * D), 0.5, 3.0)
    section_table = normal_values(arg_keys[5], (BLOCKS, 3, D), 0.5, 3.0, ((0, 2),), jnp.float32)
    value_weight = normal_values(arg_keys[6], (BLOCKS, D, H), D ** -0.5, 0.15625, ((0, 2),))
    proj_weight = normal_values(arg_keys[7], (BLOCKS, H, D), H ** -0.5, 0.15625, ((0, 2),))
    return {"inputs": inputs, "out_grad": out_grad, "guide_bin": guide_bin, "time_step": time_step, "guide_table": guide_table, "section_table": section_table, "value_weight": value_weight, "proj_weight": proj_weight}


NORM_FLOOR = 0.1

def normalize(hidden):
    centre = lax.optimization_barrier(jnp.mean(hidden, axis=-1, keepdims=True))
    centred = hidden - centre
    spread = lax.optimization_barrier(jnp.mean(centred * centred, axis=-1, keepdims=True))
    inverse = lax.rsqrt(spread + NORM_FLOOR)
    return (centred * inverse, inverse)

def conditions(guide_bin, time_step, guide_table):
    total = guide_table.shape[1]
    half = total // 2
    frequency = jnp.exp(-math.log(10000.0) * jnp.arange(half, dtype=jnp.float32) / half)
    angle = time_step.astype(jnp.float32)[..., None] * frequency
    waves = jnp.concatenate([jnp.sin(angle), jnp.cos(angle)], axis=-1)
    return guide_table.astype(jnp.float32)[guide_bin] + 0.5 * waves

def forward_block(block_in, modulation, value_weight, proj_weight):
    width = block_in.shape[1]
    hidden = block_in.astype(jnp.float32)
    normed, inverse = normalize(hidden)
    shift = modulation[:, :width]
    scale = modulation[:, width:2 * width]
    gate = modulation[:, 2 * width:]
    modulated = (normed * (1.0 + scale) + shift).astype(jnp.bfloat16)
    values = jnp.dot(modulated, value_weight, preferred_element_type=jnp.float32).astype(jnp.bfloat16)
    projected = jnp.dot(values, proj_weight, preferred_element_type=jnp.float32)
    block_out = (hidden + gate * projected).astype(jnp.bfloat16)
    return (block_out, modulated, values, projected)

def backward_block(block_in, modulated, values, projected, upstream, modulation, value_weight, proj_weight):
    width = block_in.shape[1]
    hidden = block_in.astype(jnp.float32)
    normed, inverse = normalize(hidden)
    scale = modulation[:, width:2 * width]
    gate = modulation[:, 2 * width:]
    grad_up = upstream.astype(jnp.float32)
    grad_proj = (gate * grad_up).astype(jnp.bfloat16)
    part_proj = jnp.dot(values.T, grad_proj, preferred_element_type=jnp.float32)
    grad_values = jnp.dot(grad_proj, proj_weight.T, preferred_element_type=jnp.float32).astype(jnp.bfloat16)
    part_value = jnp.dot(modulated.T, grad_values, preferred_element_type=jnp.float32)
    grad_mod = jnp.dot(grad_values, value_weight.T, preferred_element_type=jnp.float32)
    part_table = jnp.stack([lax.optimization_barrier(jnp.sum(grad_mod, axis=0)), lax.optimization_barrier(jnp.sum(grad_mod * normed, axis=0)), lax.optimization_barrier(jnp.sum(grad_up * projected, axis=0))])
    grad_norm = grad_mod * (1.0 + scale)
    centre_grad = lax.optimization_barrier(jnp.mean(grad_norm, axis=-1, keepdims=True))
    cross = lax.optimization_barrier(jnp.mean(grad_norm * normed, axis=-1, keepdims=True))
    grad_in = grad_up + inverse * (grad_norm - centre_grad - normed * cross)
    return (grad_in.astype(jnp.bfloat16), part_value, part_proj, part_table)

def reference(inputs, out_grad, guide_bin, time_step, guide_table, section_table, value_weight, proj_weight):
    condition = conditions(guide_bin, time_step, guide_table)
    rows_per = TOKENS // SAMPLES
    saved = []
    shared_all = []
    for batch in range(MICRO):
        shared = jnp.repeat(condition[batch], rows_per, axis=0)
        shared_all.append(shared)
        block_in = inputs[batch]
        kept = []
        for block in range(BLOCKS):
            modulation = shared + section_table[block].reshape(-1)
            kept.append(block_in)
            block_in = forward_block(block_in, modulation, value_weight[block], proj_weight[block])[0]
        saved.append(kept)
    value_sums = [jnp.zeros((D, H), jnp.float32) for index in range(BLOCKS)]
    proj_sums = [jnp.zeros((H, D), jnp.float32) for index in range(BLOCKS)]
    table_sums = [jnp.zeros((3, D), jnp.float32) for index in range(BLOCKS)]
    for batch in range(MICRO):
        upstream = out_grad[batch]
        for block in range(BLOCKS - 1, -1, -1):
            modulation = shared_all[batch] + section_table[block].reshape(-1)
            block_in = saved[batch][block]
            block_out, modulated, values, projected = forward_block(block_in, modulation, value_weight[block], proj_weight[block])
            upstream, part_value, part_proj, part_table = backward_block(block_in, modulated, values, projected, upstream, modulation, value_weight[block], proj_weight[block])
            value_sums[block] = value_sums[block] + part_value
            proj_sums[block] = proj_sums[block] + part_proj
            table_sums[block] = table_sums[block] + part_table
    return (jnp.stack(value_sums), jnp.stack(proj_sums), jnp.stack(table_sums))
```

```python
import functools
import math

import jax
import jax.numpy as jnp
from jax import lax
from jax.experimental import pallas as pl
from jax.experimental.pallas import tpu as pltpu
from jax.sharding import PartitionSpec as P

NORM_FLOOR = 0.1
PIECE_ROWS = 64


def shifted(value, axis, steps):
    count = lax.axis_size(axis)
    leading, last = (max(0, -steps), min(count, count - steps))
    return lax.ppermute(value, axis, [(source, source + steps) for source in range(leading, last)])


def normalize(hidden):
    centre = jnp.mean(hidden, axis=-1, keepdims=True)
    centred = hidden - centre
    spread = jnp.mean(centred * centred, axis=-1, keepdims=True)
    inverse = lax.rsqrt(spread + NORM_FLOOR)
    return (centred * inverse, inverse)


def conditions(guide_bin, time_step, guide_table):
    total = guide_table.shape[1]
    half = total // 2
    frequency = jnp.exp(-math.log(10000.0) * jnp.arange(half, dtype=jnp.float32) / half)
    angle = time_step.astype(jnp.float32)[..., None] * frequency
    waves = jnp.concatenate([jnp.sin(angle), jnp.cos(angle)], axis=-1)
    bin_count = guide_table.shape[0]
    onehot = (guide_bin[..., None] == jnp.arange(bin_count, dtype=jnp.int32)).astype(jnp.float32)
    picked = jnp.einsum(
        "msb,bw->msw", onehot, guide_table.astype(jnp.float32), precision=lax.Precision.HIGHEST
    )
    return picked + 0.5 * waves


def contract_rows(left, right):
    return lax.dot_general(
        left, right, (((0,), (0,)), ((), ())), preferred_element_type=jnp.float32
    )


def forward_block(block_in, modulation, value_weight, proj_weight):
    width = block_in.shape[1]
    hidden = block_in.astype(jnp.float32)
    normed, inverse = normalize(hidden)
    shift = modulation[:, :width]
    scale = modulation[:, width : 2 * width]
    gate = modulation[:, 2 * width :]
    modulated = (normed * (1.0 + scale) + shift).astype(jnp.bfloat16)
    values = jnp.dot(modulated, value_weight, preferred_element_type=jnp.float32).astype(
        jnp.bfloat16
    )
    projected = jnp.dot(values, proj_weight, preferred_element_type=jnp.float32)
    block_out = (hidden + gate * projected).astype(jnp.bfloat16)
    return (block_out, modulated, values, projected)


def backward_block(block_in, projected, upstream, modulation, value_weight, proj_weight):
    width = block_in.shape[1]
    hidden = block_in.astype(jnp.float32)
    normed, inverse = normalize(hidden)
    scale = modulation[:, width : 2 * width]
    gate = modulation[:, 2 * width :]
    grad_up = upstream.astype(jnp.float32)
    grad_proj = (gate * grad_up).astype(jnp.bfloat16)
    grad_values = lax.dot_general(
        grad_proj, proj_weight, (((1,), (1,)), ((), ())), preferred_element_type=jnp.float32
    ).astype(jnp.bfloat16)
    grad_mod = lax.dot_general(
        grad_values, value_weight, (((1,), (1,)), ((), ())), preferred_element_type=jnp.float32
    )
    part_table = jnp.stack(
        [
            jnp.sum(grad_mod, axis=0),
            jnp.sum(grad_mod * normed, axis=0),
            jnp.sum(grad_up * projected, axis=0),
        ]
    )
    grad_norm = grad_mod * (1.0 + scale)
    centre_grad = jnp.mean(grad_norm, axis=-1, keepdims=True)
    cross = jnp.mean(grad_norm * normed, axis=-1, keepdims=True)
    grad_in = grad_up + inverse * (grad_norm - centre_grad - normed * cross)
    return (grad_in.astype(jnp.bfloat16), grad_values, grad_proj, part_table)


def per_device_scan(
    inputs, out_grad, guide_bin, time_step, guide_table, section_table, value_weight, proj_weight
):
    sections = lax.axis_size("section")
    section_id = lax.axis_index("section")
    position = lax.axis_index("dp")
    group_size = lax.axis_size("dp")
    tok_dev = inputs.shape[1]
    width = inputs.shape[2]
    value_width = value_weight.shape[2]
    batches = inputs.shape[0]
    samples = guide_bin.shape[1]
    tokens = tok_dev * group_size
    rows_per = tokens // samples
    parts = 1
    unit_rows = tok_dev // parts
    units = batches * parts
    condition = conditions(guide_bin, time_step, guide_table)
    weights_value = value_weight[0]
    weights_proj = proj_weight[0]
    section_row = section_table[0].reshape(-1)
    sample_ids = jnp.arange(samples, dtype=jnp.int32)

    def unit_modulation(unit_id):
        batch_id = unit_id // parts
        piece_id = unit_id % parts
        chosen = lax.dynamic_index_in_dim(condition, batch_id, 0, keepdims=False)
        global_rows = (
            position * tok_dev + piece_id * unit_rows + jnp.arange(unit_rows, dtype=jnp.int32)
        )
        owner = global_rows // rows_per
        onehot = (owner[:, None] == sample_ids[None, :]).astype(jnp.float32)
        picked = jnp.dot(
            onehot, chosen, precision=lax.Precision.HIGHEST, preferred_element_type=jnp.float32
        )
        return picked + section_row

    slots = units + 1
    keep_in = jnp.zeros((slots, unit_rows, width), jnp.bfloat16)
    keep_mod = jnp.zeros((slots, unit_rows, width), jnp.bfloat16)
    keep_val = jnp.zeros((slots, unit_rows, value_width), jnp.bfloat16)
    keep_proj = jnp.zeros((slots, unit_rows, width), jnp.float32)
    arriving = jnp.zeros((unit_rows, width), jnp.bfloat16)

    def forward_tick(carry, tick_id):
        incoming, saved_in, saved_mod, saved_val, saved_proj = carry
        unit_id = tick_id - section_id
        valid = (unit_id >= 0) & (unit_id < units)
        clipped = jnp.clip(unit_id, 0, units - 1)
        first = lax.dynamic_index_in_dim(inputs, clipped, 0, keepdims=False)
        block_in = jnp.where(section_id == 0, first, incoming)

        def forward_active(operand):
            return forward_block(operand, unit_modulation(clipped), weights_value, weights_proj)

        def forward_resting(operand):
            return (
                jnp.zeros_like(operand),
                jnp.zeros_like(operand),
                jnp.zeros((unit_rows, value_width), jnp.bfloat16),
                jnp.zeros((unit_rows, width), jnp.float32),
            )

        block_out, modulated, values, projected = lax.cond(
            valid, forward_active, forward_resting, block_in
        )
        slot_id = jnp.where(valid, unit_id, units)
        saved_in = lax.dynamic_update_index_in_dim(saved_in, block_in, slot_id, 0)
        saved_mod = lax.dynamic_update_index_in_dim(saved_mod, modulated, slot_id, 0)
        saved_val = lax.dynamic_update_index_in_dim(saved_val, values, slot_id, 0)
        saved_proj = lax.dynamic_update_index_in_dim(saved_proj, projected, slot_id, 0)
        sent = shifted(block_out, "section", 1)
        return ((sent, saved_in, saved_mod, saved_val, saved_proj), None)

    ticks = jnp.arange(units + sections - 1, dtype=jnp.int32)
    carry, unused = lax.scan(
        forward_tick, (arriving, keep_in, keep_mod, keep_val, keep_proj), ticks
    )
    arriving, keep_in, keep_mod, keep_val, keep_proj = carry
    store = jnp.zeros((slots, unit_rows, value_width), jnp.bfloat16)
    extra_zero = jnp.zeros((unit_rows, value_width), jnp.bfloat16)
    keep_grad = jnp.zeros((slots, unit_rows, width), jnp.bfloat16)
    proj_sum = jnp.zeros((value_width, width), jnp.float32)
    table_sum = jnp.zeros((3, width), jnp.float32)

    def backward_tick(carry, tick_id):
        incoming, store_now, grads_now, proj_now, table_now = carry
        unit_id = tick_id - (sections - 1 - section_id)
        valid = (unit_id >= 0) & (unit_id < units)
        clipped = jnp.clip(unit_id, 0, units - 1)
        last = lax.dynamic_index_in_dim(out_grad, clipped, 0, keepdims=False)
        upstream = jnp.where(section_id == sections - 1, last, incoming)
        block_in = lax.dynamic_index_in_dim(keep_in, clipped, 0, keepdims=False)
        modulated = lax.dynamic_index_in_dim(keep_mod, clipped, 0, keepdims=False)
        values = lax.dynamic_index_in_dim(keep_val, clipped, 0, keepdims=False)
        projected = lax.dynamic_index_in_dim(keep_proj, clipped, 0, keepdims=False)

        def backward_active(operand):
            grad_in, grad_values, grad_proj, part_table = backward_block(
                block_in, projected, operand, unit_modulation(clipped), weights_value, weights_proj
            )
            part_proj = jnp.zeros((value_width, width), jnp.float32)
            return (grad_in, grad_values, grad_proj, part_proj, part_table)

        def backward_resting(operand):
            return (
                jnp.zeros_like(operand),
                extra_zero,
                jnp.zeros((unit_rows, width), jnp.bfloat16),
                jnp.zeros((value_width, width), jnp.float32),
                jnp.zeros((3, width), jnp.float32),
            )

        grad_in, extra, grad_proj, part_proj, part_table = lax.cond(
            valid, backward_active, backward_resting, upstream
        )
        slot_id = jnp.where(valid, unit_id, units)
        store_now = lax.dynamic_update_index_in_dim(store_now, extra, slot_id, 0)
        grads_now = lax.dynamic_update_index_in_dim(grads_now, grad_proj, slot_id, 0)
        sent = shifted(grad_in, "section", -1)
        return ((sent, store_now, grads_now, proj_now + part_proj, table_now + part_table), None)

    carry, unused = lax.scan(
        backward_tick, (arriving, store, keep_grad, proj_sum, table_sum), ticks
    )
    arriving, store, keep_grad, proj_sum, table_sum = carry
    mod_rows = keep_mod[:units].reshape(units * unit_rows, width)
    grad_rows = store[:units].reshape(units * unit_rows, value_width)
    columns = mod_rows
    value_part = lax.psum_scatter(
        contract_rows(columns, grad_rows), "dp", scatter_dimension=0, tiled=True
    )
    val_rows = keep_val[:units].reshape(units * unit_rows, value_width)
    upper_rows = keep_grad[:units].reshape(units * unit_rows, width)
    columns = val_rows
    proj_part = lax.psum_scatter(
        contract_rows(columns, upper_rows), "dp", scatter_dimension=0, tiled=True
    )
    table_part = lax.psum_scatter(table_sum, "dp", scatter_dimension=1, tiled=True)
    return (value_part[None], proj_part[None], table_part[None])


MESH = pl.DeviceIdType.MESH


def step_kernel(far, bin_ref, time_ref, guide_ref, section_ref, x_hbm, up_hbm, wv_hbm, wp_hbm,
                value_out, proj_out, table_out,
                x_s, up_s, wv_s, wp_s, rows_s, arrive_s, send_s, mod_s, val_s, left_s, right_s,
                proj_s, gm_s, tab_s, core_out, core_in, own_s, side_out, side_in, low_in, high_in,
                tables_s, tables_in, load_sem, hop_send, hop_recv, core_send, core_recv,
                side_send, side_recv, low_send, low_recv, high_send, high_recv,
                table_send, table_recv):
    units, unit_rows = x_hbm.shape[0], x_hbm.shape[1]
    count, width = x_s.shape
    depth = wv_s.shape[1]
    hops = hop_send.shape[0]
    piece = count // hops
    chunk = math.gcd(piece, 32)
    group = 4 * far
    section = lax.axis_index("section")
    me = lax.axis_index("dp")
    core, side, place = me % 2, (me // 2) % 2, me // 4

    barrier = pltpu.get_barrier_semaphore()
    pl.semaphore_signal(
        barrier, inc=1, device_id={"section": 1 - section}, device_id_type=MESH
    )
    for step in range(1, group):
        pl.semaphore_signal(
            barrier, inc=1, device_id={"dp": (me + step) % group}, device_id_type=MESH
        )

    loads = [
        pltpu.make_async_copy(wv_hbm.at[0], wv_s, load_sem.at[0]),
        pltpu.make_async_copy(wp_hbm.at[0], wp_s, load_sem.at[1]),
    ]
    for unit in range(units):
        part = pl.ds(unit * unit_rows, unit_rows)
        loads.append(pltpu.make_async_copy(x_hbm.at[unit], x_s.at[part], load_sem.at[2 + unit]))
    for unit in range(units):
        part = pl.ds(unit * unit_rows, unit_rows)
        loads.append(
            pltpu.make_async_copy(up_hbm.at[unit], up_s.at[part], load_sem.at[2 + units + unit])
        )
    for load in [loads[2], loads[0], loads[1]] + loads[3:]:
        load.start()

    total = guide_ref.shape[1]
    half = total // 2
    samples = bin_ref.shape[1]
    sample = (me * unit_rows) // (unit_rows * group // samples)
    lane = lax.broadcasted_iota(jnp.int32, (units, half), 1).astype(jnp.float32)
    frequency = jnp.exp(-math.log(10000.0) * lane / half)
    which = lax.broadcasted_iota(jnp.int32, (units, half), 0)
    times = jnp.zeros((units, half), jnp.float32)
    for unit in range(units):
        times = jnp.where(which == unit, time_ref[unit, sample].astype(jnp.float32), times)
    angle = times * frequency
    waves = jnp.concatenate([jnp.sin(angle), jnp.cos(angle)], axis=1)
    table = guide_ref[...].astype(jnp.float32)
    bins = lax.broadcasted_iota(jnp.int32, table.shape, 0)
    for unit in range(units):
        picked = jnp.sum(
            jnp.where(bins == bin_ref[unit, sample], table, 0.0), axis=0, keepdims=True
        )
        picked = picked + 0.5 * waves[unit:unit + 1]
        for index in range(3):
            lanes = slice(index * width, (index + 1) * width)
            rows_s[unit, index] = picked[:, lanes] + section_ref[0, index:index + 1]
    tab_s[...] = jnp.zeros_like(tab_s)

    def hop(index):
        part = pl.ds(pl.multiple_of(index * piece, piece), piece)
        return pltpu.make_async_remote_copy(
            src_ref=send_s.at[part],
            dst_ref=arrive_s.at[part],
            send_sem=hop_send.at[index],
            recv_sem=hop_recv.at[index],
            device_id={"section": 1 - section},
            device_id_type=MESH,
        )

    def each_chunk(start, size, body):
        @pl.loop(0, size // chunk)
        def step(index):
            body(pl.ds(pl.multiple_of(start + index * chunk, chunk), chunk), index * chunk)

    def multiply(size, body):
        tile = math.gcd(size, 768)

        @pl.loop(0, size // tile)
        def step(index):
            body(pl.ds(pl.multiple_of(index * tile, tile), tile))

    def add_rows(index, value):
        tab_s[index] += jnp.sum(value.reshape(chunk // 8, 8, width), axis=0)

    def forward(index, source, send):
        start = pl.multiple_of(index * piece, piece)
        unit = start // unit_rows
        rows = pl.ds(start, piece)

        def modulate(part, unused):
            normed, inverse = normalize(source[part].astype(jnp.float32))
            scaled = normed * (1.0 + rows_s[unit, 1]) + rows_s[unit, 0]
            mod_s[part] = scaled.astype(jnp.bfloat16)

        def first_dot(part):
            val_s[rows, part] = jnp.dot(
                mod_s[rows], wv_s[:, part], preferred_element_type=jnp.float32
            ).astype(jnp.bfloat16)

        def second_dot(part):
            proj_s[rows, part] = jnp.dot(
                val_s[rows], wp_s[:, part], preferred_element_type=jnp.float32
            )

        def add_gated(part, unused):
            hidden = source[part].astype(jnp.float32)
            block_out = hidden + rows_s[unit, 2] * proj_s[part]
            send_s[part] = block_out.astype(jnp.bfloat16)

        each_chunk(start, piece, modulate)
        multiply(depth, first_dot)
        multiply(width, second_dot)
        if send:
            each_chunk(start, piece, add_gated)

    def gated(index, upstream):
        start = pl.multiple_of(index * piece, piece)
        unit = start // unit_rows

        def body(part, unused):
            grad_up = upstream[part].astype(jnp.float32)
            right_s[0, part] = (rows_s[unit, 2] * grad_up).astype(jnp.bfloat16)
            add_rows(2, grad_up * proj_s[part])

        each_chunk(start, piece, body)

    def to_values(index):
        rows = pl.ds(pl.multiple_of(index * piece, piece), piece)

        def body(part):
            right_s[1, rows, part] = lax.dot_general(
                right_s[0, rows], wp_s[part, :], (((1,), (1,)), ((), ())),
                preferred_element_type=jnp.float32,
            ).astype(jnp.bfloat16)

        multiply(depth, body)

    def to_input(start, size, source, upstream):
        start = pl.multiple_of(start, size)
        unit = start // unit_rows
        rows = pl.ds(start, size)

        def dot(part):
            gm_s[pl.ds(0, size), part] = lax.dot_general(
                right_s[1, rows], wv_s[part, :], (((1,), (1,)), ((), ())),
                preferred_element_type=jnp.float32,
            )

        def body(part, offset):
            normed, inverse = normalize(source[part].astype(jnp.float32))
            grad_mod = gm_s[pl.ds(pl.multiple_of(offset, chunk), chunk)]
            add_rows(0, grad_mod)
            add_rows(1, grad_mod * normed)
            if upstream is not None:
                grad_norm = grad_mod * (1.0 + rows_s[unit, 1])
                centre_grad = jnp.mean(grad_norm, axis=-1, keepdims=True)
                cross = jnp.mean(grad_norm * normed, axis=-1, keepdims=True)
                grad_up = upstream[part].astype(jnp.float32)
                grad_in = grad_up + inverse * (grad_norm - centre_grad - normed * cross)
                send_s[part] = grad_in.astype(jnp.bfloat16)

        multiply(width, dot)
        each_chunk(start, size, body)

    def turn_left(unit):
        part = pl.ds(pl.multiple_of(unit * unit_rows, unit_rows), unit_rows)
        left_s[0, :, part] = val_s[part].T
        left_s[1, :, part] = mod_s[part].T

    @pl.when(section == 0)
    def earlier():
        for load in loads[2:2 + units]:
            load.wait()
        loads[0].wait()
        loads[1].wait()
        pl.semaphore_wait(barrier, group)

        @pl.loop(0, hops)
        def out(index):
            forward(index, x_s, True)
            hop(index).start()

        @pl.loop(0, units)
        def turn(unit):
            turn_left(unit)

        for load in loads[2 + units:]:
            load.wait()

        @pl.loop(0, hops)
        def back(index):
            hop(index).wait_recv()
            gated(index, arrive_s)
            to_values(index)

    @pl.when(section == 1)
    def later():
        for load in loads:
            load.wait()
        pl.semaphore_wait(barrier, group)

        @pl.loop(0, hops)
        def both(index):
            hop(index).wait_recv()
            forward(index, arrive_s, False)
            gated(index, up_s)
            to_values(index)
            to_input(index * piece, piece, arrive_s, up_s)
            hop(index).start()

        @pl.loop(0, units)
        def turn(unit):
            turn_left(unit)

    ranks = [sorted(range(far), key=lambda block: -abs(block - spot)) for spot in range(far)]
    order = [(0, rank) for rank in range(far - 1)] + [(1, rank) for rank in range(far - 1)]
    order = order + [(0, far - 1), (1, far - 1)]
    pieces = len(order)
    block_rows = left_s.shape[1] // group
    per_matrix = far - 1

    def chosen(values):
        result = 0
        for spot in range(far):
            away = (place - spot + far) % far
            result = result + values[spot] * (1 - (away + far - 1) // far)
        return result

    blocks = [chosen([ranks[spot][rank] for spot in range(far)]) for rank in range(far)]

    def partial(turn, index):
        matrix, rank = order[index]
        which = (1 - side) if turn == 0 else side
        first = pl.multiple_of((blocks[rank] * 2 + which) * 2 * block_rows, 2 * block_rows)
        product = jnp.dot(
            left_s[matrix, pl.ds(first, 2 * block_rows)], right_s[matrix],
            preferred_element_type=jnp.float32,
        ).astype(jnp.bfloat16)
        kept = side_out if turn == 0 else own_s

        @pl.when(core == 0)
        def even():
            kept[index] = product[:block_rows]
            core_out[turn, index] = product[block_rows:]

        @pl.when(core == 1)
        def odd():
            kept[index] = product[block_rows:]
            core_out[turn, index] = product[:block_rows]

    def core_copy(turn, index):
        return pltpu.make_async_remote_copy(
            src_ref=core_out.at[turn, index],
            dst_ref=core_in.at[turn, index],
            send_sem=core_send.at[turn, index],
            recv_sem=core_recv.at[turn, index],
            device_id={"dp": me + 1 - 2 * core},
            device_id_type=MESH,
        )

    def side_copy(index):
        return pltpu.make_async_remote_copy(
            src_ref=side_out.at[index],
            dst_ref=side_in.at[index],
            send_sem=side_send.at[index],
            recv_sem=side_recv.at[index],
            device_id={"dp": me + 2 - 4 * side},
            device_id_type=MESH,
        )

    def over_block(body):
        tall = math.gcd(block_rows, 16)

        @pl.loop(0, block_rows // tall)
        def step(at):
            body(pl.ds(pl.multiple_of(at * tall, tall), tall))

    def send_side(index):
        core_copy(0, index).wait_recv()

        def add(part):
            mine = side_out[index, part].astype(jnp.float32)
            mine = mine + core_in[0, index, part].astype(jnp.float32)
            side_out[index, part] = mine.astype(jnp.bfloat16)

        over_block(add)
        side_copy(index).start()

    for index in range(pieces):
        partial(0, index)
        core_copy(0, index).start()
        if index > 0:
            send_side(index - 1)
    for index in range(pieces):
        partial(1, index)
        core_copy(1, index).start()
        if index == 0:
            send_side(pieces - 1)

    def up_copy(matrix, block):
        return pltpu.make_async_remote_copy(
            src_ref=own_s.at[order.index((matrix, rank_of(block)))],
            dst_ref=low_in.at[matrix, block],
            send_sem=low_send.at[matrix, block],
            recv_sem=low_recv.at[matrix, block],
            device_id={"dp": (me + 4) % group},
            device_id_type=MESH,
        )

    def down_copy(matrix, block):
        return pltpu.make_async_remote_copy(
            src_ref=own_s.at[order.index((matrix, rank_of(block)))],
            dst_ref=high_in.at[matrix, block],
            send_sem=high_send.at[matrix, block],
            recv_sem=high_recv.at[matrix, block],
            device_id={"dp": (me + group - 4) % group},
            device_id_type=MESH,
        )

    spot_now = [0]

    def rank_of(block):
        return ranks[spot_now[0]].index(block)

    def chain(spot, indices):
        spot_now[0] = spot
        for index in indices:
            matrix, rank = order[index]
            block = ranks[spot][rank]
            core_copy(1, index).wait_recv()
            side_copy(index).wait_recv()
            terms = []
            if block >= spot and spot > 0:
                up_copy(matrix, block).wait_recv()
                terms.append(low_in)
            if block <= spot and spot < far - 1:
                down_copy(matrix, block).wait_recv()
                terms.append(high_in)

            def add(part):
                mine = own_s[index, part].astype(jnp.float32)
                mine = mine + core_in[1, index, part].astype(jnp.float32)
                mine = mine + side_in[index, part].astype(jnp.float32)
                for term in terms:
                    mine = mine + term[matrix, block, part].astype(jnp.float32)
                if block == spot:
                    (proj_out, value_out)[matrix][part] = mine
                else:
                    own_s[index, part] = mine.astype(jnp.bfloat16)

            over_block(add)
            if block > spot:
                up_copy(matrix, block).start()
            elif block < spot:
                down_copy(matrix, block).start()

    def finish(spot):
        spot_now[0] = spot
        for matrix in range(2):
            for block in range(far):
                if block > spot:
                    up_copy(matrix, block).wait_send()
                elif block < spot:
                    down_copy(matrix, block).wait_send()

    def stage(indices):
        for spot in range(far):
            @pl.when(place == spot)
            def run(spot=spot):
                chain(spot, indices)

    stage(range(0, 1))

    @pl.when(section == 0)
    def rest():
        @pl.loop(0, units)
        def one(unit):
            to_input(unit * unit_rows, unit_rows, x_s, None)

    lanes = table_out.shape[1]
    table = jnp.concatenate(
        [jnp.sum(tab_s[index], axis=0, keepdims=True) for index in range(3)]
        + [jnp.zeros((5, width), jnp.float32)], axis=0,
    )
    for owner in range(group):
        tables_s[owner, :, :lanes] = table[:, owner * lanes:(owner + 1) * lanes]

    def table_copy(step):
        return pltpu.make_async_remote_copy(
            src_ref=tables_s.at[(me + step) % group],
            dst_ref=tables_in.at[step - 1],
            send_sem=table_send.at[step - 1],
            recv_sem=table_recv.at[step - 1],
            device_id={"dp": (me + step) % group},
            device_id_type=MESH,
        )

    for step in range(1, group):
        table_copy(step).start()
    stage(range(1, pieces))
    sums = tables_s[me]
    for step in range(1, group):
        table_copy(step).wait_recv()
        sums = sums + tables_in[step - 1]
    table_out[...] = sums[:, :lanes]

    @pl.loop(0, hops)
    def sent(index):
        hop(index).wait_send()

    for index in range(pieces):
        core_copy(0, index).wait_send()
        core_copy(1, index).wait_send()
        side_copy(index).wait_send()
    for step in range(1, group):
        table_copy(step).wait_send()
    for spot in range(far):
        @pl.when(place == spot)
        def drain(spot=spot):
            finish(spot)


def per_device(
    inputs, out_grad, guide_bin, time_step, guide_table, section_table, value_weight, proj_weight
):
    units, rows, width = inputs.shape
    depth = value_weight.shape[2]
    group = lax.axis_size("dp")
    per_sample = rows * group // guide_bin.shape[1]
    if (lax.axis_size("section") != 2 or group % 4 or per_sample % rows or rows % 128
            or width != depth or width % (group * 16)):
        return per_device_scan(
            inputs, out_grad, guide_bin, time_step, guide_table, section_table,
            value_weight, proj_weight,
        )
    far = group // 4
    count = units * rows
    piece = PIECE_ROWS
    hops = count // piece
    block = (width // group, width)
    pieces = 2 * far
    lanes = width // group
    vmem = pl.BlockSpec(memory_space=pltpu.VMEM)
    smem = pl.BlockSpec(memory_space=pltpu.SMEM)
    hbm = pl.BlockSpec(memory_space=pl.ANY)
    dma = pltpu.SemaphoreType.DMA
    half = jnp.bfloat16
    value_sum, proj_sum, table_sum = pl.pallas_call(
        functools.partial(step_kernel, far),
        out_shape=(
            jax.ShapeDtypeStruct(block, jnp.float32),
            jax.ShapeDtypeStruct(block, jnp.float32),
            jax.ShapeDtypeStruct((8, lanes), jnp.float32),
        ),
        in_specs=[smem, smem, vmem, vmem, hbm, hbm, hbm, hbm],
        out_specs=(vmem,) * 3,
        scratch_shapes=[
            pltpu.VMEM((count, width), half),
            pltpu.VMEM((count, width), half),
            pltpu.VMEM((width, depth), half),
            pltpu.VMEM((depth, width), half),
            pltpu.VMEM((units, 3, 1, width), jnp.float32),
            pltpu.VMEM((count, width), half),
            pltpu.VMEM((count, width), half),
            pltpu.VMEM((count, width), half),
            pltpu.VMEM((count, depth), half),
            pltpu.VMEM((2, width, count), half),
            pltpu.VMEM((2, count, width), half),
            pltpu.VMEM((count, width), jnp.float32),
            pltpu.VMEM((rows, width), jnp.float32),
            pltpu.VMEM((3, 8, width), jnp.float32),
            pltpu.VMEM((2, pieces) + block, half),
            pltpu.VMEM((2, pieces) + block, half),
            pltpu.VMEM((pieces,) + block, half),
            pltpu.VMEM((pieces,) + block, half),
            pltpu.VMEM((pieces,) + block, half),
            pltpu.VMEM((2, far) + block, half),
            pltpu.VMEM((2, far) + block, half),
            pltpu.VMEM((group, 8, 128), jnp.float32),
            pltpu.VMEM((group - 1, 8, 128), jnp.float32),
            dma((2 + 2 * units,)), dma((hops,)), dma((hops,)), dma((2, pieces)), dma((2, pieces)),
            dma((pieces,)), dma((pieces,)), dma((2, far)), dma((2, far)), dma((2, far)),
            dma((2, far)), dma((group - 1,)), dma((group - 1,)),
        ],
        compiler_params=pltpu.CompilerParams(
            collective_id=0, has_side_effects=True, vmem_limit_bytes=62 * 1024 * 1024
        ),
    )(
        guide_bin, time_step, guide_table, section_table, inputs, out_grad,
        value_weight, proj_weight,
    )
    return (value_sum[None], proj_sum[None], table_sum[None, :3])


def solution(mesh):
    return jax.shard_map(
        per_device,
        mesh=mesh,
        in_specs=(
            P(None, "dp", None),
            P(None, "dp", None),
            P(),
            P(),
            P(),
            P("section", None, None),
            P("section", None, None),
            P("section", None, None),
        ),
        out_specs=(P("section", "dp", None), P("section", "dp", None), P("section", None, "dp")),
        check_vma=False,
    )
```

```python
import functools
import math

import jax
import jax.numpy as jnp
from jax import lax
from jax.experimental import pallas as pl
from jax.experimental.pallas import tpu as pltpu
from jax.sharding import PartitionSpec as P

NORM_FLOOR = 0.1
PIECE_ROWS = 32
FORWARD_ROWS = 64
CHUNK_ROWS = 16
UNROLL = 2
TILE = 1536


def shifted(value, axis, steps):
    count = lax.axis_size(axis)
    leading, last = (max(0, -steps), min(count, count - steps))
    return lax.ppermute(value, axis, [(source, source + steps) for source in range(leading, last)])


def normalize(hidden):
    centre = jnp.mean(hidden, axis=-1, keepdims=True)
    centred = hidden - centre
    spread = jnp.mean(centred * centred, axis=-1, keepdims=True)
    inverse = lax.rsqrt(spread + NORM_FLOOR)
    return (centred * inverse, inverse)


def conditions(guide_bin, time_step, guide_table):
    total = guide_table.shape[1]
    half = total // 2
    frequency = jnp.exp(-math.log(10000.0) * jnp.arange(half, dtype=jnp.float32) / half)
    angle = time_step.astype(jnp.float32)[..., None] * frequency
    waves = jnp.concatenate([jnp.sin(angle), jnp.cos(angle)], axis=-1)
    bin_count = guide_table.shape[0]
    onehot = (guide_bin[..., None] == jnp.arange(bin_count, dtype=jnp.int32)).astype(jnp.float32)
    picked = jnp.einsum(
        "msb,bw->msw", onehot, guide_table.astype(jnp.float32), precision=lax.Precision.HIGHEST
    )
    return picked + 0.5 * waves


def contract_rows(left, right):
    return lax.dot_general(
        left, right, (((0,), (0,)), ((), ())), preferred_element_type=jnp.float32
    )


def forward_block(block_in, modulation, value_weight, proj_weight):
    width = block_in.shape[1]
    hidden = block_in.astype(jnp.float32)
    normed, inverse = normalize(hidden)
    shift = modulation[:, :width]
    scale = modulation[:, width : 2 * width]
    gate = modulation[:, 2 * width :]
    modulated = (normed * (1.0 + scale) + shift).astype(jnp.bfloat16)
    values = jnp.dot(modulated, value_weight, preferred_element_type=jnp.float32).astype(
        jnp.bfloat16
    )
    projected = jnp.dot(values, proj_weight, preferred_element_type=jnp.float32)
    block_out = (hidden + gate * projected).astype(jnp.bfloat16)
    return (block_out, modulated, values, projected)


def backward_block(block_in, projected, upstream, modulation, value_weight, proj_weight):
    width = block_in.shape[1]
    hidden = block_in.astype(jnp.float32)
    normed, inverse = normalize(hidden)
    scale = modulation[:, width : 2 * width]
    gate = modulation[:, 2 * width :]
    grad_up = upstream.astype(jnp.float32)
    grad_proj = (gate * grad_up).astype(jnp.bfloat16)
    grad_values = lax.dot_general(
        grad_proj, proj_weight, (((1,), (1,)), ((), ())), preferred_element_type=jnp.float32
    ).astype(jnp.bfloat16)
    grad_mod = lax.dot_general(
        grad_values, value_weight, (((1,), (1,)), ((), ())), preferred_element_type=jnp.float32
    )
    part_table = jnp.stack(
        [
            jnp.sum(grad_mod, axis=0),
            jnp.sum(grad_mod * normed, axis=0),
            jnp.sum(grad_up * projected, axis=0),
        ]
    )
    grad_norm = grad_mod * (1.0 + scale)
    centre_grad = jnp.mean(grad_norm, axis=-1, keepdims=True)
    cross = jnp.mean(grad_norm * normed, axis=-1, keepdims=True)
    grad_in = grad_up + inverse * (grad_norm - centre_grad - normed * cross)
    return (grad_in.astype(jnp.bfloat16), grad_values, grad_proj, part_table)


def per_device_scan(
    inputs, out_grad, guide_bin, time_step, guide_table, section_table, value_weight, proj_weight
):
    sections = lax.axis_size("section")
    section_id = lax.axis_index("section")
    position = lax.axis_index("dp")
    group_size = lax.axis_size("dp")
    tok_dev = inputs.shape[1]
    width = inputs.shape[2]
    value_width = value_weight.shape[2]
    batches = inputs.shape[0]
    samples = guide_bin.shape[1]
    tokens = tok_dev * group_size
    rows_per = tokens // samples
    parts = 1
    unit_rows = tok_dev // parts
    units = batches * parts
    condition = conditions(guide_bin, time_step, guide_table)
    weights_value = value_weight[0]
    weights_proj = proj_weight[0]
    section_row = section_table[0].reshape(-1)
    sample_ids = jnp.arange(samples, dtype=jnp.int32)

    def unit_modulation(unit_id):
        batch_id = unit_id // parts
        piece_id = unit_id % parts
        chosen = lax.dynamic_index_in_dim(condition, batch_id, 0, keepdims=False)
        global_rows = (
            position * tok_dev + piece_id * unit_rows + jnp.arange(unit_rows, dtype=jnp.int32)
        )
        owner = global_rows // rows_per
        onehot = (owner[:, None] == sample_ids[None, :]).astype(jnp.float32)
        picked = jnp.dot(
            onehot, chosen, precision=lax.Precision.HIGHEST, preferred_element_type=jnp.float32
        )
        return picked + section_row

    slots = units + 1
    keep_in = jnp.zeros((slots, unit_rows, width), jnp.bfloat16)
    keep_mod = jnp.zeros((slots, unit_rows, width), jnp.bfloat16)
    keep_val = jnp.zeros((slots, unit_rows, value_width), jnp.bfloat16)
    keep_proj = jnp.zeros((slots, unit_rows, width), jnp.float32)
    arriving = jnp.zeros((unit_rows, width), jnp.bfloat16)

    def forward_tick(carry, tick_id):
        incoming, saved_in, saved_mod, saved_val, saved_proj = carry
        unit_id = tick_id - section_id
        valid = (unit_id >= 0) & (unit_id < units)
        clipped = jnp.clip(unit_id, 0, units - 1)
        first = lax.dynamic_index_in_dim(inputs, clipped, 0, keepdims=False)
        block_in = jnp.where(section_id == 0, first, incoming)

        def forward_active(operand):
            return forward_block(operand, unit_modulation(clipped), weights_value, weights_proj)

        def forward_resting(operand):
            return (
                jnp.zeros_like(operand),
                jnp.zeros_like(operand),
                jnp.zeros((unit_rows, value_width), jnp.bfloat16),
                jnp.zeros((unit_rows, width), jnp.float32),
            )

        block_out, modulated, values, projected = lax.cond(
            valid, forward_active, forward_resting, block_in
        )
        slot_id = jnp.where(valid, unit_id, units)
        saved_in = lax.dynamic_update_index_in_dim(saved_in, block_in, slot_id, 0)
        saved_mod = lax.dynamic_update_index_in_dim(saved_mod, modulated, slot_id, 0)
        saved_val = lax.dynamic_update_index_in_dim(saved_val, values, slot_id, 0)
        saved_proj = lax.dynamic_update_index_in_dim(saved_proj, projected, slot_id, 0)
        sent = shifted(block_out, "section", 1)
        return ((sent, saved_in, saved_mod, saved_val, saved_proj), None)

    ticks = jnp.arange(units + sections - 1, dtype=jnp.int32)
    carry, unused = lax.scan(
        forward_tick, (arriving, keep_in, keep_mod, keep_val, keep_proj), ticks
    )
    arriving, keep_in, keep_mod, keep_val, keep_proj = carry
    store = jnp.zeros((slots, unit_rows, value_width), jnp.bfloat16)
    extra_zero = jnp.zeros((unit_rows, value_width), jnp.bfloat16)
    keep_grad = jnp.zeros((slots, unit_rows, width), jnp.bfloat16)
    proj_sum = jnp.zeros((value_width, width), jnp.float32)
    table_sum = jnp.zeros((3, width), jnp.float32)

    def backward_tick(carry, tick_id):
        incoming, store_now, grads_now, proj_now, table_now = carry
        unit_id = tick_id - (sections - 1 - section_id)
        valid = (unit_id >= 0) & (unit_id < units)
        clipped = jnp.clip(unit_id, 0, units - 1)
        last = lax.dynamic_index_in_dim(out_grad, clipped, 0, keepdims=False)
        upstream = jnp.where(section_id == sections - 1, last, incoming)
        block_in = lax.dynamic_index_in_dim(keep_in, clipped, 0, keepdims=False)
        modulated = lax.dynamic_index_in_dim(keep_mod, clipped, 0, keepdims=False)
        values = lax.dynamic_index_in_dim(keep_val, clipped, 0, keepdims=False)
        projected = lax.dynamic_index_in_dim(keep_proj, clipped, 0, keepdims=False)

        def backward_active(operand):
            grad_in, grad_values, grad_proj, part_table = backward_block(
                block_in, projected, operand, unit_modulation(clipped), weights_value, weights_proj
            )
            part_proj = jnp.zeros((value_width, width), jnp.float32)
            return (grad_in, grad_values, grad_proj, part_proj, part_table)

        def backward_resting(operand):
            return (
                jnp.zeros_like(operand),
                extra_zero,
                jnp.zeros((unit_rows, width), jnp.bfloat16),
                jnp.zeros((value_width, width), jnp.float32),
                jnp.zeros((3, width), jnp.float32),
            )

        grad_in, extra, grad_proj, part_proj, part_table = lax.cond(
            valid, backward_active, backward_resting, upstream
        )
        slot_id = jnp.where(valid, unit_id, units)
        store_now = lax.dynamic_update_index_in_dim(store_now, extra, slot_id, 0)
        grads_now = lax.dynamic_update_index_in_dim(grads_now, grad_proj, slot_id, 0)
        sent = shifted(grad_in, "section", -1)
        return ((sent, store_now, grads_now, proj_now + part_proj, table_now + part_table), None)

    carry, unused = lax.scan(
        backward_tick, (arriving, store, keep_grad, proj_sum, table_sum), ticks
    )
    arriving, store, keep_grad, proj_sum, table_sum = carry
    mod_rows = keep_mod[:units].reshape(units * unit_rows, width)
    grad_rows = store[:units].reshape(units * unit_rows, value_width)
    columns = mod_rows
    value_part = lax.psum_scatter(
        contract_rows(columns, grad_rows), "dp", scatter_dimension=0, tiled=True
    )
    val_rows = keep_val[:units].reshape(units * unit_rows, value_width)
    upper_rows = keep_grad[:units].reshape(units * unit_rows, width)
    columns = val_rows
    proj_part = lax.psum_scatter(
        contract_rows(columns, upper_rows), "dp", scatter_dimension=0, tiled=True
    )
    table_part = lax.psum_scatter(table_sum, "dp", scatter_dimension=1, tiled=True)
    return (value_part[None], proj_part[None], table_part[None])


MESH = pl.DeviceIdType.MESH


def step_kernel(far, bin_ref, time_ref, guide_ref, section_ref, x_hbm, up_hbm, wv_hbm, wp_hbm,
                value_out, proj_out, table_out,
                local_s, wv_s, wp_s, rows_s, arrive_s, send_s, mod_s, val_s, left_s, right_s,
                wide_s, part_s, tab_s, core_out, core_in, own_s, side_out, side_in, low_in, high_in,
                tables_s, tables_in, load_sem, hop_send, hop_recv, core_send, core_recv,
                side_send, side_recv, low_send, low_recv, high_send, high_recv,
                table_send, table_recv):
    units, unit_rows = x_hbm.shape[0], x_hbm.shape[1]
    count, width = local_s.shape
    depth = wv_s.shape[1]
    hops = hop_send.shape[0]
    piece = count // hops
    per_unit = unit_rows // piece
    group = 4 * far
    section = lax.axis_index("section")
    me = lax.axis_index("dp")
    core, side, place = me % 2, (me // 2) % 2, me // 4

    barrier = pltpu.get_barrier_semaphore()
    pl.semaphore_signal(
        barrier, inc=1, device_id={"section": 1 - section}, device_id_type=MESH
    )
    for step in range(1, group):
        pl.semaphore_signal(
            barrier, inc=1, device_id={"dp": (me + step) % group}, device_id_type=MESH
        )

    def load_rows(source, unit):
        part = pl.ds(unit * unit_rows, unit_rows)
        return pltpu.make_async_copy(source.at[unit], local_s.at[part], load_sem.at[2 + unit])

    load_value = pltpu.make_async_copy(wv_hbm.at[0], wv_s, load_sem.at[0])
    load_proj = pltpu.make_async_copy(wp_hbm.at[0], wp_s, load_sem.at[1])

    @pl.when(section == 0)
    def load_first():
        load_rows(x_hbm, 0).start()
        load_value.start()
        load_proj.start()
        for unit in range(1, units):
            load_rows(x_hbm, unit).start()

    @pl.when(section == 1)
    def load_last():
        load_rows(up_hbm, 0).start()
        load_proj.start()
        load_value.start()
        for unit in range(1, units):
            load_rows(up_hbm, unit).start()

    total = guide_ref.shape[1]
    half = total // 2
    samples = bin_ref.shape[0] // units
    sample = (me * unit_rows) // (unit_rows * group // samples)
    lane = lax.broadcasted_iota(jnp.int32, (units, half), 1).astype(jnp.float32)
    frequency = jnp.exp(-math.log(10000.0) * lane / half)
    which = lax.broadcasted_iota(jnp.int32, (units, half), 0)
    times = jnp.zeros((units, half), jnp.float32)
    for unit in range(units):
        time = time_ref[unit * samples + sample].astype(jnp.float32)
        times = jnp.where(which == unit, time, times)
    angle = times * frequency
    waves = jnp.concatenate([jnp.sin(angle), jnp.cos(angle)], axis=1)
    table = guide_ref[...].astype(jnp.float32)
    bins = lax.broadcasted_iota(jnp.int32, table.shape, 0)
    for unit in range(units):
        picked = jnp.sum(
            jnp.where(bins == bin_ref[unit * samples + sample], table, 0.0),
            axis=0, keepdims=True,
        )
        picked = picked + 0.5 * waves[unit:unit + 1]
        for index in range(3):
            lanes = slice(index * width, (index + 1) * width)
            rows_s[unit, index] = picked[:, lanes] + section_ref[index]
    tab_s[...] = jnp.zeros_like(tab_s)

    def hop(index):
        part = pl.ds(pl.multiple_of(index * piece, piece), piece)
        return pltpu.make_async_remote_copy(
            src_ref=send_s.at[part],
            dst_ref=arrive_s.at[part],
            send_sem=hop_send.at[index],
            recv_sem=hop_recv.at[index],
            device_id={"section": 1 - section},
            device_id_type=MESH,
        )

    def each_chunk(start, size, body):
        tall = math.gcd(size, CHUNK_ROWS)

        @pl.loop(0, size // tall, unroll=min(UNROLL, size // tall))
        def step(index):
            body(pl.ds(pl.multiple_of(start + index * tall, tall), tall), index * tall)

    def multiply(size, body):
        tile = math.gcd(size, TILE)

        @pl.loop(0, size // tile)
        def step(index):
            body(pl.ds(pl.multiple_of(index * tile, tile), tile))

    def add_rows(index, value):
        rows = value.shape[0]
        tab_s[index] += jnp.sum(value.reshape(rows // 8, 8, width), axis=0)

    def to_depth(rows, part):
        val_s[rows, part] = jnp.dot(
            mod_s[rows], wv_s[:, part], preferred_element_type=jnp.float32
        ).astype(jnp.bfloat16)

    def to_width(rows, part):
        return jnp.dot(val_s[rows], wp_s[:, part], preferred_element_type=jnp.float32)

    def to_values(rows):
        def body(part):
            right_s[1, rows, part] = lax.dot_general(
                right_s[0, rows], wp_s[part, :], (((1,), (1,)), ((), ())),
                preferred_element_type=jnp.float32,
            ).astype(jnp.bfloat16)

        multiply(depth, body)

    def to_mod(rows, target, target_rows):
        def body(part):
            target[target_rows, part] = lax.dot_general(
                right_s[1, rows], wv_s[part, :], (((1,), (1,)), ((), ())),
                preferred_element_type=jnp.float32,
            )

        multiply(width, body)

    def unit_rows_at(unit):
        return pl.ds(pl.multiple_of(unit * unit_rows, unit_rows), unit_rows)

    def turn_left(unit):
        part = unit_rows_at(unit)
        left_s[0, :, part] = val_s[part].T
        left_s[1, :, part] = mod_s[part].T

    def forward(index, size):
        start = pl.multiple_of(index * size, size)
        unit = start // unit_rows
        rows = pl.ds(start, size)

        def modulate(part, unused):
            normed, inverse = normalize(local_s[part].astype(jnp.float32))
            scaled = normed * (1.0 + rows_s[unit, 1]) + rows_s[unit, 0]
            mod_s[part] = scaled.astype(jnp.bfloat16)

        each_chunk(start, size, modulate)
        multiply(depth, lambda part: to_depth(rows, part))

        def second(part):
            wide_s[rows, part] = to_width(rows, part)

        multiply(width, second)

        def add_gated(part, unused):
            hidden = local_s[part].astype(jnp.float32)
            block_out = hidden + rows_s[unit, 2] * wide_s[part]
            send_s[part] = block_out.astype(jnp.bfloat16)

        for at in range(size // piece):
            each_chunk(start + at * piece, piece, add_gated)
            hop(index * (size // piece) + at).start()

    def receive(index):
        start = pl.multiple_of(index * piece, piece)
        unit = start // unit_rows
        hop(index).wait_recv()

        def body(part, unused):
            grad_up = arrive_s[part].astype(jnp.float32)
            right_s[0, part] = (rows_s[unit, 2] * grad_up).astype(jnp.bfloat16)
            add_rows(2, grad_up * wide_s[part])

        each_chunk(start, piece, body)

    def table_rows(unit):
        to_mod(unit_rows_at(unit), part_s, slice(None))

        def body(part, offset):
            normed, inverse = normalize(local_s[part].astype(jnp.float32))
            grad_mod = part_s[pl.ds(offset, part.size)]
            add_rows(0, grad_mod)
            add_rows(1, grad_mod * normed)

        each_chunk(unit * unit_rows, unit_rows, body)

    @pl.when(section == 0)
    def earlier():
        load_rows(x_hbm, 0).wait()
        load_value.wait()
        load_proj.wait()
        for unit in range(1, units):
            load_rows(x_hbm, unit).wait()
        pl.semaphore_wait(barrier, group)
        size = math.gcd(unit_rows, FORWARD_ROWS)

        @pl.loop(0, count // size)
        def out(index):
            forward(index, size)

        @pl.loop(0, units)
        def back(unit):
            turn_left(unit)

            @pl.loop(0, per_unit)
            def one(at):
                receive(unit * per_unit + at)

            to_values(unit_rows_at(unit))

    def grads_ahead(unit):
        def body(part, unused):
            grad_up = local_s[part].astype(jnp.float32)
            right_s[0, part] = (rows_s[unit, 2] * grad_up).astype(jnp.bfloat16)

        each_chunk(unit * unit_rows, unit_rows, body)
        to_values(unit_rows_at(unit))

    def mods_ahead(unit):
        rows = unit_rows_at(unit)
        to_mod(rows, wide_s, rows)

    def values_behind(unit):
        multiply(depth, lambda part: to_depth(unit_rows_at(unit), part))

    def gates_behind(unit):
        rows = unit_rows_at(unit)

        def second(part):
            part_s[:, part] = to_width(rows, part)

        multiply(width, second)

        def body(part, offset):
            add_rows(2, local_s[part].astype(jnp.float32) * part_s[pl.ds(offset, part.size)])

        each_chunk(unit * unit_rows, unit_rows, body)

    def answer(index):
        start = pl.multiple_of(index * piece, piece)
        unit = start // unit_rows
        hop(index).wait_recv()

        def body(part, unused):
            normed, inverse = normalize(arrive_s[part].astype(jnp.float32))
            scale = 1.0 + rows_s[unit, 1]
            mod_s[part] = (normed * scale + rows_s[unit, 0]).astype(jnp.bfloat16)
            grad_mod = wide_s[part]
            add_rows(0, grad_mod)
            add_rows(1, grad_mod * normed)
            grad_norm = grad_mod * scale
            centre_grad = jnp.mean(grad_norm, axis=-1, keepdims=True)
            cross = jnp.mean(grad_norm * normed, axis=-1, keepdims=True)
            grad_up = local_s[part].astype(jnp.float32)
            grad_in = grad_up + inverse * (grad_norm - centre_grad - normed * cross)
            send_s[part] = grad_in.astype(jnp.bfloat16)

        each_chunk(start, piece, body)
        hop(index).start()

    @pl.when(section == 1)
    def later():
        load_rows(up_hbm, 0).wait()
        load_proj.wait()
        load_value.wait()
        for unit in range(1, units):
            load_rows(up_hbm, unit).wait()
        for unit in range(min(2, units)):
            grads_ahead(unit)
            mods_ahead(unit)
        pl.semaphore_wait(barrier, group)

        @pl.loop(0, units)
        def both(unit):
            @pl.loop(0, per_unit)
            def one(at):
                answer(unit * per_unit + at)

                @pl.when((at == 0) & (unit + 2 < units))
                def job_grads():
                    grads_ahead(unit + 2)

                @pl.when((at == 1) & (unit + 2 < units))
                def job_mods():
                    mods_ahead(unit + 2)

                @pl.when((at == 2 % per_unit) & (unit >= 1))
                def job_values():
                    values_behind(unit - 1)

                @pl.when((at == 3 % per_unit) & (unit >= 1))
                def job_gates():
                    gates_behind(unit - 1)

        values_behind(units - 1)
        gates_behind(units - 1)

        @pl.loop(0, units)
        def turn(unit):
            turn_left(unit)

    ranks = [sorted(range(far), key=lambda block: -abs(block - spot)) for spot in range(far)]
    order = [(0, rank) for rank in range(far - 1)] + [(1, rank) for rank in range(far - 1)]
    order = order + [(0, far - 1), (1, far - 1)]
    pieces = len(order)
    block_rows = left_s.shape[1] // group
    per_matrix = far - 1

    def chosen(values):
        result = 0
        for spot in range(far):
            away = (place - spot + far) % far
            result = result + values[spot] * (1 - (away + far - 1) // far)
        return result

    blocks = [chosen([ranks[spot][rank] for spot in range(far)]) for rank in range(far)]

    def partial(turn, index):
        matrix, rank = order[index]
        which = (1 - side) if turn == 0 else side
        first = pl.multiple_of((blocks[rank] * 2 + which) * 2 * block_rows, 2 * block_rows)
        product = jnp.dot(
            left_s[matrix, pl.ds(first, 2 * block_rows)], right_s[matrix],
            preferred_element_type=jnp.float32,
        ).astype(jnp.bfloat16)
        kept = side_out if turn == 0 else own_s

        @pl.when(core == 0)
        def even():
            kept[index] = product[:block_rows]
            core_out[turn, index] = product[block_rows:]

        @pl.when(core == 1)
        def odd():
            kept[index] = product[block_rows:]
            core_out[turn, index] = product[:block_rows]

    def core_copy(turn, index):
        return pltpu.make_async_remote_copy(
            src_ref=core_out.at[turn, index],
            dst_ref=core_in.at[turn, index],
            send_sem=core_send.at[turn, index],
            recv_sem=core_recv.at[turn, index],
            device_id={"dp": me + 1 - 2 * core},
            device_id_type=MESH,
        )

    def side_copy(index):
        return pltpu.make_async_remote_copy(
            src_ref=side_out.at[index],
            dst_ref=side_in.at[index],
            send_sem=side_send.at[index],
            recv_sem=side_recv.at[index],
            device_id={"dp": me + 2 - 4 * side},
            device_id_type=MESH,
        )

    def over_block(body):
        tall = math.gcd(block_rows, 16)

        @pl.loop(0, block_rows // tall)
        def step(at):
            body(pl.ds(pl.multiple_of(at * tall, tall), tall))

    def send_side(index):
        core_copy(0, index).wait_recv()

        def add(part):
            mine = side_out[index, part].astype(jnp.float32)
            mine = mine + core_in[0, index, part].astype(jnp.float32)
            side_out[index, part] = mine.astype(jnp.bfloat16)

        over_block(add)
        side_copy(index).start()

    for index in range(pieces):
        partial(0, index)
        core_copy(0, index).start()
        if index > 0:
            send_side(index - 1)
    for index in range(pieces):
        partial(1, index)
        core_copy(1, index).start()
        if index == 0:
            send_side(pieces - 1)

    def up_copy(matrix, block):
        return pltpu.make_async_remote_copy(
            src_ref=own_s.at[order.index((matrix, rank_of(block)))],
            dst_ref=low_in.at[matrix, block],
            send_sem=low_send.at[matrix, block],
            recv_sem=low_recv.at[matrix, block],
            device_id={"dp": (me + 4) % group},
            device_id_type=MESH,
        )

    def down_copy(matrix, block):
        return pltpu.make_async_remote_copy(
            src_ref=own_s.at[order.index((matrix, rank_of(block)))],
            dst_ref=high_in.at[matrix, block],
            send_sem=high_send.at[matrix, block],
            recv_sem=high_recv.at[matrix, block],
            device_id={"dp": (me + group - 4) % group},
            device_id_type=MESH,
        )

    spot_now = [0]

    def rank_of(block):
        return ranks[spot_now[0]].index(block)

    def chain(spot, indices):
        spot_now[0] = spot
        for index in indices:
            matrix, rank = order[index]
            block = ranks[spot][rank]
            core_copy(1, index).wait_recv()
            side_copy(index).wait_recv()
            terms = []
            if block >= spot and spot > 0:
                up_copy(matrix, block).wait_recv()
                terms.append(low_in)
            if block <= spot and spot < far - 1:
                down_copy(matrix, block).wait_recv()
                terms.append(high_in)

            def add(part):
                mine = own_s[index, part].astype(jnp.float32)
                mine = mine + core_in[1, index, part].astype(jnp.float32)
                mine = mine + side_in[index, part].astype(jnp.float32)
                for term in terms:
                    mine = mine + term[matrix, block, part].astype(jnp.float32)
                if block == spot:
                    (proj_out, value_out)[matrix][part] = mine
                else:
                    own_s[index, part] = mine.astype(jnp.bfloat16)

            over_block(add)
            if block > spot:
                up_copy(matrix, block).start()
            elif block < spot:
                down_copy(matrix, block).start()

    def finish(spot):
        spot_now[0] = spot
        for matrix in range(2):
            for block in range(far):
                if block > spot:
                    up_copy(matrix, block).wait_send()
                elif block < spot:
                    down_copy(matrix, block).wait_send()

    def stage(indices):
        for spot in range(far):
            @pl.when(place == spot)
            def run(spot=spot):
                chain(spot, indices)

    ahead = min(units, pieces - 1)
    for index in range(ahead):
        stage([index])

        @pl.when(section == 0)
        def tables(index=index):
            for unit in range(index, units if index == ahead - 1 else index + 1):
                table_rows(unit)

    lanes = table_out.shape[2]
    table = jnp.concatenate(
        [jnp.sum(tab_s[index], axis=0, keepdims=True) for index in range(3)]
        + [jnp.zeros((5, width), jnp.float32)], axis=0,
    )
    for owner in range(group):
        tables_s[owner, :, :lanes] = table[:, owner * lanes:(owner + 1) * lanes]

    def table_copy(step):
        return pltpu.make_async_remote_copy(
            src_ref=tables_s.at[(me + step) % group],
            dst_ref=tables_in.at[step - 1],
            send_sem=table_send.at[step - 1],
            recv_sem=table_recv.at[step - 1],
            device_id={"dp": (me + step) % group},
            device_id_type=MESH,
        )

    for step in range(1, group):
        table_copy(step).start()
    stage(range(ahead, pieces))
    sums = tables_s[me]
    for step in range(1, group):
        table_copy(step).wait_recv()
        sums = sums + tables_in[step - 1]
    for index in range(3):
        table_out[index] = sums[index:index + 1, :lanes]

    @pl.loop(0, hops)
    def sent(index):
        hop(index).wait_send()

    for index in range(pieces):
        core_copy(0, index).wait_send()
        core_copy(1, index).wait_send()
        side_copy(index).wait_send()
    for step in range(1, group):
        table_copy(step).wait_send()
    for spot in range(far):
        @pl.when(place == spot)
        def drain(spot=spot):
            finish(spot)


def per_device(
    inputs, out_grad, guide_bin, time_step, guide_table, section_table, value_weight, proj_weight
):
    units, rows, width = inputs.shape
    depth = value_weight.shape[2]
    group = lax.axis_size("dp")
    per_sample = rows * group // guide_bin.shape[1]
    if (lax.axis_size("section") != 2 or group % 4 or per_sample % rows or rows % 128
            or width != depth or width % (group * 16)):
        return per_device_scan(
            inputs, out_grad, guide_bin, time_step, guide_table, section_table,
            value_weight, proj_weight,
        )
    far = group // 4
    count = units * rows
    piece = math.gcd(rows, PIECE_ROWS)
    hops = count // piece
    block = (width // group, width)
    pieces = 2 * far
    lanes = width // group
    vmem = pl.BlockSpec(memory_space=pltpu.VMEM)
    smem = pl.BlockSpec(memory_space=pltpu.SMEM)
    hbm = pl.BlockSpec(memory_space=pl.ANY)
    dma = pltpu.SemaphoreType.DMA
    half = jnp.bfloat16
    value_sum, proj_sum, table_sum = pl.pallas_call(
        functools.partial(step_kernel, far),
        out_shape=(
            jax.ShapeDtypeStruct(block, jnp.float32),
            jax.ShapeDtypeStruct(block, jnp.float32),
            jax.ShapeDtypeStruct((3, 1, lanes), jnp.float32),
        ),
        in_specs=[smem, smem, vmem, vmem, hbm, hbm, hbm, hbm],
        out_specs=(vmem,) * 3,
        scratch_shapes=[
            pltpu.VMEM((count, width), half),
            pltpu.VMEM((width, depth), half),
            pltpu.VMEM((depth, width), half),
            pltpu.VMEM((units, 3, 1, width), jnp.float32),
            pltpu.VMEM((count, width), half),
            pltpu.VMEM((count, width), half),
            pltpu.VMEM((count, width), half),
            pltpu.VMEM((count, depth), half),
            pltpu.VMEM((2, width, count), half),
            pltpu.VMEM((2, count, width), half),
            pltpu.VMEM((count, width), jnp.float32),
            pltpu.VMEM((rows, width), jnp.float32),
            pltpu.VMEM((3, 8, width), jnp.float32),
            pltpu.VMEM((2, pieces) + block, half),
            pltpu.VMEM((2, pieces) + block, half),
            pltpu.VMEM((pieces,) + block, half),
            pltpu.VMEM((pieces,) + block, half),
            pltpu.VMEM((pieces,) + block, half),
            pltpu.VMEM((2, far) + block, half),
            pltpu.VMEM((2, far) + block, half),
            pltpu.VMEM((group, 8, 128), jnp.float32),
            pltpu.VMEM((group - 1, 8, 128), jnp.float32),
            dma((2 + units,)), dma((hops,)), dma((hops,)), dma((2, pieces)), dma((2, pieces)),
            dma((pieces,)), dma((pieces,)), dma((2, far)), dma((2, far)), dma((2, far)),
            dma((2, far)), dma((group - 1,)), dma((group - 1,)),
        ],
        compiler_params=pltpu.CompilerParams(
            collective_id=0, has_side_effects=True, vmem_limit_bytes=62 * 1024 * 1024
        ),
    )(
        guide_bin.reshape(-1), time_step.reshape(-1), guide_table,
        section_table.transpose(1, 0, 2), inputs, out_grad,
        value_weight, proj_weight,
    )
    return (value_sum[None], proj_sum[None], table_sum.transpose(1, 0, 2))


def solution(mesh):
    return jax.shard_map(
        per_device,
        mesh=mesh,
        in_specs=(
            P(None, "dp", None),
            P(None, "dp", None),
            P(),
            P(),
            P(),
            P("section", None, None),
            P("section", None, None),
            P("section", None, None),
        ),
        out_specs=(P("section", "dp", None), P("section", "dp", None), P("section", None, "dp")),
        check_vma=False,
    )
```

```python
import functools
import math

import jax
import jax.numpy as jnp
from jax import lax
from jax.experimental import pallas as pl
from jax.experimental.pallas import tpu as pltpu
from jax.sharding import PartitionSpec as P

NORM_FLOOR = 0.1
PIECE_ROWS = 32
FORWARD_ROWS = 64
CHUNK_ROWS = 16
UNROLL = 2
TILE = 1536
OWN_DEEP = 2


def shifted(value, axis, steps):
    count = lax.axis_size(axis)
    leading, last = (max(0, -steps), min(count, count - steps))
    return lax.ppermute(value, axis, [(source, source + steps) for source in range(leading, last)])


def normalize(hidden):
    centre = jnp.mean(hidden, axis=-1, keepdims=True)
    centred = hidden - centre
    spread = jnp.mean(centred * centred, axis=-1, keepdims=True)
    inverse = lax.rsqrt(spread + NORM_FLOOR)
    return (centred * inverse, inverse)


def conditions(guide_bin, time_step, guide_table):
    total = guide_table.shape[1]
    half = total // 2
    frequency = jnp.exp(-math.log(10000.0) * jnp.arange(half, dtype=jnp.float32) / half)
    angle = time_step.astype(jnp.float32)[..., None] * frequency
    waves = jnp.concatenate([jnp.sin(angle), jnp.cos(angle)], axis=-1)
    bin_count = guide_table.shape[0]
    onehot = (guide_bin[..., None] == jnp.arange(bin_count, dtype=jnp.int32)).astype(jnp.float32)
    picked = jnp.einsum(
        "msb,bw->msw", onehot, guide_table.astype(jnp.float32), precision=lax.Precision.HIGHEST
    )
    return picked + 0.5 * waves


def contract_rows(left, right):
    return lax.dot_general(
        left, right, (((0,), (0,)), ((), ())), preferred_element_type=jnp.float32
    )


def forward_block(block_in, modulation, value_weight, proj_weight):
    width = block_in.shape[1]
    hidden = block_in.astype(jnp.float32)
    normed, inverse = normalize(hidden)
    shift = modulation[:, :width]
    scale = modulation[:, width : 2 * width]
    gate = modulation[:, 2 * width :]
    modulated = (normed * (1.0 + scale) + shift).astype(jnp.bfloat16)
    values = jnp.dot(modulated, value_weight, preferred_element_type=jnp.float32).astype(
        jnp.bfloat16
    )
    projected = jnp.dot(values, proj_weight, preferred_element_type=jnp.float32)
    block_out = (hidden + gate * projected).astype(jnp.bfloat16)
    return (block_out, modulated, values, projected)


def backward_block(block_in, projected, upstream, modulation, value_weight, proj_weight):
    width = block_in.shape[1]
    hidden = block_in.astype(jnp.float32)
    normed, inverse = normalize(hidden)
    scale = modulation[:, width : 2 * width]
    gate = modulation[:, 2 * width :]
    grad_up = upstream.astype(jnp.float32)
    grad_proj = (gate * grad_up).astype(jnp.bfloat16)
    grad_values = lax.dot_general(
        grad_proj, proj_weight, (((1,), (1,)), ((), ())), preferred_element_type=jnp.float32
    ).astype(jnp.bfloat16)
    grad_mod = lax.dot_general(
        grad_values, value_weight, (((1,), (1,)), ((), ())), preferred_element_type=jnp.float32
    )
    part_table = jnp.stack(
        [
            jnp.sum(grad_mod, axis=0),
            jnp.sum(grad_mod * normed, axis=0),
            jnp.sum(grad_up * projected, axis=0),
        ]
    )
    grad_norm = grad_mod * (1.0 + scale)
    centre_grad = jnp.mean(grad_norm, axis=-1, keepdims=True)
    cross = jnp.mean(grad_norm * normed, axis=-1, keepdims=True)
    grad_in = grad_up + inverse * (grad_norm - centre_grad - normed * cross)
    return (grad_in.astype(jnp.bfloat16), grad_values, grad_proj, part_table)


def per_device_scan(
    inputs, out_grad, guide_bin, time_step, guide_table, section_table, value_weight, proj_weight
):
    sections = lax.axis_size("section")
    section_id = lax.axis_index("section")
    position = lax.axis_index("dp")
    group_size = lax.axis_size("dp")
    tok_dev = inputs.shape[1]
    width = inputs.shape[2]
    value_width = value_weight.shape[2]
    batches = inputs.shape[0]
    samples = guide_bin.shape[1]
    tokens = tok_dev * group_size
    rows_per = tokens // samples
    parts = 1
    unit_rows = tok_dev // parts
    units = batches * parts
    condition = conditions(guide_bin, time_step, guide_table)
    weights_value = value_weight[0]
    weights_proj = proj_weight[0]
    section_row = section_table[0].reshape(-1)
    sample_ids = jnp.arange(samples, dtype=jnp.int32)

    def unit_modulation(unit_id):
        batch_id = unit_id // parts
        piece_id = unit_id % parts
        chosen = lax.dynamic_index_in_dim(condition, batch_id, 0, keepdims=False)
        global_rows = (
            position * tok_dev + piece_id * unit_rows + jnp.arange(unit_rows, dtype=jnp.int32)
        )
        owner = global_rows // rows_per
        onehot = (owner[:, None] == sample_ids[None, :]).astype(jnp.float32)
        picked = jnp.dot(
            onehot, chosen, precision=lax.Precision.HIGHEST, preferred_element_type=jnp.float32
        )
        return picked + section_row

    slots = units + 1
    keep_in = jnp.zeros((slots, unit_rows, width), jnp.bfloat16)
    keep_mod = jnp.zeros((slots, unit_rows, width), jnp.bfloat16)
    keep_val = jnp.zeros((slots, unit_rows, value_width), jnp.bfloat16)
    keep_proj = jnp.zeros((slots, unit_rows, width), jnp.float32)
    arriving = jnp.zeros((unit_rows, width), jnp.bfloat16)

    def forward_tick(carry, tick_id):
        incoming, saved_in, saved_mod, saved_val, saved_proj = carry
        unit_id = tick_id - section_id
        valid = (unit_id >= 0) & (unit_id < units)
        clipped = jnp.clip(unit_id, 0, units - 1)
        first = lax.dynamic_index_in_dim(inputs, clipped, 0, keepdims=False)
        block_in = jnp.where(section_id == 0, first, incoming)

        def forward_active(operand):
            return forward_block(operand, unit_modulation(clipped), weights_value, weights_proj)

        def forward_resting(operand):
            return (
                jnp.zeros_like(operand),
                jnp.zeros_like(operand),
                jnp.zeros((unit_rows, value_width), jnp.bfloat16),
                jnp.zeros((unit_rows, width), jnp.float32),
            )

        block_out, modulated, values, projected = lax.cond(
            valid, forward_active, forward_resting, block_in
        )
        slot_id = jnp.where(valid, unit_id, units)
        saved_in = lax.dynamic_update_index_in_dim(saved_in, block_in, slot_id, 0)
        saved_mod = lax.dynamic_update_index_in_dim(saved_mod, modulated, slot_id, 0)
        saved_val = lax.dynamic_update_index_in_dim(saved_val, values, slot_id, 0)
        saved_proj = lax.dynamic_update_index_in_dim(saved_proj, projected, slot_id, 0)
        sent = shifted(block_out, "section", 1)
        return ((sent, saved_in, saved_mod, saved_val, saved_proj), None)

    ticks = jnp.arange(units + sections - 1, dtype=jnp.int32)
    carry, unused = lax.scan(
        forward_tick, (arriving, keep_in, keep_mod, keep_val, keep_proj), ticks
    )
    arriving, keep_in, keep_mod, keep_val, keep_proj = carry
    store = jnp.zeros((slots, unit_rows, value_width), jnp.bfloat16)
    extra_zero = jnp.zeros((unit_rows, value_width), jnp.bfloat16)
    keep_grad = jnp.zeros((slots, unit_rows, width), jnp.bfloat16)
    proj_sum = jnp.zeros((value_width, width), jnp.float32)
    table_sum = jnp.zeros((3, width), jnp.float32)

    def backward_tick(carry, tick_id):
        incoming, store_now, grads_now, proj_now, table_now = carry
        unit_id = tick_id - (sections - 1 - section_id)
        valid = (unit_id >= 0) & (unit_id < units)
        clipped = jnp.clip(unit_id, 0, units - 1)
        last = lax.dynamic_index_in_dim(out_grad, clipped, 0, keepdims=False)
        upstream = jnp.where(section_id == sections - 1, last, incoming)
        block_in = lax.dynamic_index_in_dim(keep_in, clipped, 0, keepdims=False)
        modulated = lax.dynamic_index_in_dim(keep_mod, clipped, 0, keepdims=False)
        values = lax.dynamic_index_in_dim(keep_val, clipped, 0, keepdims=False)
        projected = lax.dynamic_index_in_dim(keep_proj, clipped, 0, keepdims=False)

        def backward_active(operand):
            grad_in, grad_values, grad_proj, part_table = backward_block(
                block_in, projected, operand, unit_modulation(clipped), weights_value, weights_proj
            )
            part_proj = jnp.zeros((value_width, width), jnp.float32)
            return (grad_in, grad_values, grad_proj, part_proj, part_table)

        def backward_resting(operand):
            return (
                jnp.zeros_like(operand),
                extra_zero,
                jnp.zeros((unit_rows, width), jnp.bfloat16),
                jnp.zeros((value_width, width), jnp.float32),
                jnp.zeros((3, width), jnp.float32),
            )

        grad_in, extra, grad_proj, part_proj, part_table = lax.cond(
            valid, backward_active, backward_resting, upstream
        )
        slot_id = jnp.where(valid, unit_id, units)
        store_now = lax.dynamic_update_index_in_dim(store_now, extra, slot_id, 0)
        grads_now = lax.dynamic_update_index_in_dim(grads_now, grad_proj, slot_id, 0)
        sent = shifted(grad_in, "section", -1)
        return ((sent, store_now, grads_now, proj_now + part_proj, table_now + part_table), None)

    carry, unused = lax.scan(
        backward_tick, (arriving, store, keep_grad, proj_sum, table_sum), ticks
    )
    arriving, store, keep_grad, proj_sum, table_sum = carry
    mod_rows = keep_mod[:units].reshape(units * unit_rows, width)
    grad_rows = store[:units].reshape(units * unit_rows, value_width)
    columns = mod_rows
    value_part = lax.psum_scatter(
        contract_rows(columns, grad_rows), "dp", scatter_dimension=0, tiled=True
    )
    val_rows = keep_val[:units].reshape(units * unit_rows, value_width)
    upper_rows = keep_grad[:units].reshape(units * unit_rows, width)
    columns = val_rows
    proj_part = lax.psum_scatter(
        contract_rows(columns, upper_rows), "dp", scatter_dimension=0, tiled=True
    )
    table_part = lax.psum_scatter(table_sum, "dp", scatter_dimension=1, tiled=True)
    return (value_part[None], proj_part[None], table_part[None])


MESH = pl.DeviceIdType.MESH


def step_kernel(far, bin_ref, time_ref, guide_ref, section_ref, x_hbm, up_hbm, wv_hbm, wp_hbm,
                value_out, proj_out, table_out,
                local_s, wv_s, wp_s, rows_s, arrive_s, send_s, mod_s, val_s, left_s, right_s,
                wide_s, part_s, tab_s, core_out, core_in, kept_s, side_out, side_in, low_in, high_in,
                deep_s, deep_low, deep_high, cross_out, cross_in,
                tables_s, tables_in, load_sem, hop_send, hop_recv, core_send, core_recv,
                side_send, side_recv, low_send, low_recv, high_send, high_recv,
                down_send, down_recv, rise_send, rise_recv, cross_send, cross_recv,
                table_send, table_recv):
    units, unit_rows = x_hbm.shape[0], x_hbm.shape[1]
    count, width = local_s.shape
    depth = wv_s.shape[1]
    hops = hop_send.shape[0]
    piece = count // hops
    per_unit = unit_rows // piece
    group = 4 * far
    section = lax.axis_index("section")
    me = lax.axis_index("dp")
    core, side, place = me % 2, (me // 2) % 2, me // 4

    barrier = pltpu.get_barrier_semaphore()
    pl.semaphore_signal(
        barrier, inc=1, device_id={"section": 1 - section}, device_id_type=MESH
    )
    for step in range(1, group):
        pl.semaphore_signal(
            barrier, inc=1, device_id={"dp": (me + step) % group}, device_id_type=MESH
        )

    def load_rows(source, unit):
        part = pl.ds(unit * unit_rows, unit_rows)
        return pltpu.make_async_copy(source.at[unit], local_s.at[part], load_sem.at[2 + unit])

    load_value = pltpu.make_async_copy(wv_hbm.at[0], wv_s, load_sem.at[0])
    load_proj = pltpu.make_async_copy(wp_hbm.at[0], wp_s, load_sem.at[1])

    @pl.when(section == 0)
    def load_first():
        load_rows(x_hbm, 0).start()
        load_value.start()
        load_proj.start()
        for unit in range(1, units):
            load_rows(x_hbm, unit).start()

    @pl.when(section == 1)
    def load_last():
        load_rows(up_hbm, 0).start()
        load_proj.start()
        load_value.start()
        for unit in range(1, units):
            load_rows(up_hbm, unit).start()

    total = guide_ref.shape[1]
    half = total // 2
    samples = bin_ref.shape[0] // units
    sample = (me * unit_rows) // (unit_rows * group // samples)
    lane = lax.broadcasted_iota(jnp.int32, (units, half), 1).astype(jnp.float32)
    frequency = jnp.exp(-math.log(10000.0) * lane / half)
    which = lax.broadcasted_iota(jnp.int32, (units, half), 0)
    times = jnp.zeros((units, half), jnp.float32)
    for unit in range(units):
        time = time_ref[unit * samples + sample].astype(jnp.float32)
        times = jnp.where(which == unit, time, times)
    angle = times * frequency
    waves = jnp.concatenate([jnp.sin(angle), jnp.cos(angle)], axis=1)
    table = guide_ref[...].astype(jnp.float32)
    bins = lax.broadcasted_iota(jnp.int32, table.shape, 0)
    for unit in range(units):
        picked = jnp.sum(
            jnp.where(bins == bin_ref[unit * samples + sample], table, 0.0),
            axis=0, keepdims=True,
        )
        picked = picked + 0.5 * waves[unit:unit + 1]
        for index in range(3):
            lanes = slice(index * width, (index + 1) * width)
            rows_s[unit, index] = picked[:, lanes] + section_ref[index]
    tab_s[...] = jnp.zeros_like(tab_s)

    def hop(index):
        part = pl.ds(pl.multiple_of(index * piece, piece), piece)
        return pltpu.make_async_remote_copy(
            src_ref=send_s.at[part],
            dst_ref=arrive_s.at[part],
            send_sem=hop_send.at[index],
            recv_sem=hop_recv.at[index],
            device_id={"section": 1 - section},
            device_id_type=MESH,
        )

    def each_chunk(start, size, body):
        tall = math.gcd(size, CHUNK_ROWS)

        @pl.loop(0, size // tall, unroll=min(UNROLL, size // tall))
        def step(index):
            body(pl.ds(pl.multiple_of(start + index * tall, tall), tall), index * tall)

    def multiply(size, body):
        tile = math.gcd(size, TILE)

        @pl.loop(0, size // tile)
        def step(index):
            body(pl.ds(pl.multiple_of(index * tile, tile), tile))

    def add_rows(index, value):
        rows = value.shape[0]
        tab_s[index] += jnp.sum(value.reshape(rows // 8, 8, width), axis=0)

    def to_depth(rows, part):
        val_s[rows, part] = jnp.dot(
            mod_s[rows], wv_s[:, part], preferred_element_type=jnp.float32
        ).astype(jnp.bfloat16)

    def to_width(rows, part):
        return jnp.dot(val_s[rows], wp_s[:, part], preferred_element_type=jnp.float32)

    def to_values(rows):
        def body(part):
            right_s[1, rows, part] = lax.dot_general(
                right_s[0, rows], wp_s[part, :], (((1,), (1,)), ((), ())),
                preferred_element_type=jnp.float32,
            ).astype(jnp.bfloat16)

        multiply(depth, body)

    def to_mod(rows, target, target_rows):
        def body(part):
            target[target_rows, part] = lax.dot_general(
                right_s[1, rows], wv_s[part, :], (((1,), (1,)), ((), ())),
                preferred_element_type=jnp.float32,
            )

        multiply(width, body)

    def unit_rows_at(unit):
        return pl.ds(pl.multiple_of(unit * unit_rows, unit_rows), unit_rows)

    def turn_left(unit):
        part = unit_rows_at(unit)
        left_s[0, :, part] = val_s[part].T
        left_s[1, :, part] = mod_s[part].T

    def forward(index, size):
        start = pl.multiple_of(index * size, size)
        unit = start // unit_rows
        rows = pl.ds(start, size)

        def modulate(part, unused):
            normed, inverse = normalize(local_s[part].astype(jnp.float32))
            scaled = normed * (1.0 + rows_s[unit, 1]) + rows_s[unit, 0]
            mod_s[part] = scaled.astype(jnp.bfloat16)

        each_chunk(start, size, modulate)
        multiply(depth, lambda part: to_depth(rows, part))

        @pl.when(index == 0)
        def load_second():
            load_proj.wait()

        def second(part):
            wide_s[rows, part] = to_width(rows, part)

        multiply(width, second)

        @pl.when(index == 0)
        def enter():
            for unit in range(1, units):
                load_rows(x_hbm, unit).wait()
            pl.semaphore_wait(barrier, group)

        def add_gated(part, unused):
            hidden = local_s[part].astype(jnp.float32)
            block_out = hidden + rows_s[unit, 2] * wide_s[part]
            send_s[part] = block_out.astype(jnp.bfloat16)

        for at in range(size // piece):
            each_chunk(start + at * piece, piece, add_gated)
            hop(index * (size // piece) + at).start()

    def receive(index):
        start = pl.multiple_of(index * piece, piece)
        unit = start // unit_rows
        hop(index).wait_recv()

        def body(part, unused):
            grad_up = arrive_s[part].astype(jnp.float32)
            right_s[0, part] = (rows_s[unit, 2] * grad_up).astype(jnp.bfloat16)
            add_rows(2, grad_up * wide_s[part])

        each_chunk(start, piece, body)

    def table_rows(unit):
        to_mod(unit_rows_at(unit), part_s, slice(None))

        def body(part, offset):
            normed, inverse = normalize(local_s[part].astype(jnp.float32))
            grad_mod = part_s[pl.ds(offset, part.size)]
            add_rows(0, grad_mod)
            add_rows(1, grad_mod * normed)

        each_chunk(unit * unit_rows, unit_rows, body)

    @pl.when(section == 0)
    def earlier():
        load_rows(x_hbm, 0).wait()
        load_value.wait()
        size = math.gcd(unit_rows, FORWARD_ROWS)

        @pl.loop(0, count // size)
        def out(index):
            forward(index, size)

        @pl.loop(0, units)
        def back(unit):
            turn_left(unit)

            @pl.loop(0, per_unit)
            def one(at):
                receive(unit * per_unit + at)

            @pl.when(unit < units - 1)
            def values_now():
                to_values(unit_rows_at(unit))

    def grads_ahead(unit):
        def body(part, unused):
            grad_up = local_s[part].astype(jnp.float32)
            right_s[0, part] = (rows_s[unit, 2] * grad_up).astype(jnp.bfloat16)

        each_chunk(unit * unit_rows, unit_rows, body)
        to_values(unit_rows_at(unit))

    def mods_ahead(unit):
        rows = unit_rows_at(unit)
        to_mod(rows, wide_s, rows)

    def values_behind(unit):
        multiply(depth, lambda part: to_depth(unit_rows_at(unit), part))

    def gates_behind(unit):
        rows = unit_rows_at(unit)

        def second(part):
            part_s[:, part] = to_width(rows, part)

        multiply(width, second)

        def body(part, offset):
            add_rows(2, local_s[part].astype(jnp.float32) * part_s[pl.ds(offset, part.size)])

        each_chunk(unit * unit_rows, unit_rows, body)

    def answer(index):
        start = pl.multiple_of(index * piece, piece)
        unit = start // unit_rows
        hop(index).wait_recv()

        def body(part, unused):
            normed, inverse = normalize(arrive_s[part].astype(jnp.float32))
            scale = 1.0 + rows_s[unit, 1]
            mod_s[part] = (normed * scale + rows_s[unit, 0]).astype(jnp.bfloat16)
            grad_mod = wide_s[part]
            add_rows(0, grad_mod)
            add_rows(1, grad_mod * normed)
            grad_norm = grad_mod * scale
            centre_grad = jnp.mean(grad_norm, axis=-1, keepdims=True)
            cross = jnp.mean(grad_norm * normed, axis=-1, keepdims=True)
            grad_up = local_s[part].astype(jnp.float32)
            grad_in = grad_up + inverse * (grad_norm - centre_grad - normed * cross)
            send_s[part] = grad_in.astype(jnp.bfloat16)

        each_chunk(start, piece, body)
        hop(index).start()

    @pl.when(section == 1)
    def later():
        load_rows(up_hbm, 0).wait()
        load_proj.wait()
        load_value.wait()
        for unit in range(1, units):
            load_rows(up_hbm, unit).wait()
        for unit in range(min(2, units)):
            grads_ahead(unit)
            mods_ahead(unit)
        pl.semaphore_wait(barrier, group)

        @pl.loop(0, units)
        def both(unit):
            @pl.loop(0, per_unit)
            def one(at):
                answer(unit * per_unit + at)

                @pl.when((at == 0) & (unit + 2 < units))
                def job_grads():
                    grads_ahead(unit + 2)

                @pl.when((at == 1) & (unit + 2 < units))
                def job_mods():
                    mods_ahead(unit + 2)

                @pl.when((at == 2 % per_unit) & (unit >= 1))
                def job_values():
                    values_behind(unit - 1)

                @pl.when((at == 3 % per_unit) & (unit >= 1))
                def job_gates():
                    gates_behind(unit - 1)

        values_behind(units - 1)
        gates_behind(units - 1)

        @pl.loop(0, units)
        def turn(unit):
            turn_left(unit)

    ranks = [sorted(range(far), key=lambda block: -abs(block - spot)) for spot in range(far)]
    order = [(0, rank) for rank in range(far - 1)] + [(1, rank) for rank in range(far - 1)]
    order = order + [(0, far - 1), (1, far - 1)]
    pieces = len(order)
    block_rows = left_s.shape[1] // group
    per_matrix = far - 1

    def chosen(values):
        result = 0
        for spot in range(far):
            away = (place - spot + far) % far
            result = result + values[spot] * (1 - (away + far - 1) // far)
        return result

    blocks = [chosen([ranks[spot][rank] for spot in range(far)]) for rank in range(far)]

    def partial(turn, index):
        matrix, rank = order[index]
        which = (1 - side) if turn == 0 else side
        first = pl.multiple_of((blocks[rank] * 2 + which) * 2 * block_rows, 2 * block_rows)
        product = jnp.dot(
            left_s[matrix, pl.ds(first, 2 * block_rows)], right_s[matrix],
            preferred_element_type=jnp.float32,
        ).astype(jnp.bfloat16)

        @pl.when(core == 0)
        def even():
            kept_s[turn, index] = product[:block_rows]
            core_out[turn, index] = product[block_rows:]

        @pl.when(core == 1)
        def odd():
            kept_s[turn, index] = product[block_rows:]
            core_out[turn, index] = product[:block_rows]

    def core_copy(turn, index):
        return pltpu.make_async_remote_copy(
            src_ref=core_out.at[turn, index],
            dst_ref=core_in.at[turn, index],
            send_sem=core_send.at[turn, index],
            recv_sem=core_recv.at[turn, index],
            device_id={"dp": me + 1 - 2 * core},
            device_id_type=MESH,
        )

    def side_copy(index):
        return pltpu.make_async_remote_copy(
            src_ref=side_out.at[index],
            dst_ref=side_in.at[index],
            send_sem=side_send.at[index],
            recv_sem=side_recv.at[index],
            device_id={"dp": me + 2 - 4 * side},
            device_id_type=MESH,
        )

    def over_block(body):
        tall = math.gcd(block_rows, 16)

        @pl.loop(0, block_rows // tall)
        def step(at):
            body(pl.ds(pl.multiple_of(at * tall, tall), tall))

    near = side_out.shape[2]
    near_lanes, deep_lanes = slice(0, near), slice(near, width)
    spot_now = [0]

    def rank_of(block):
        return ranks[spot_now[0]].index(block)

    def row_copy(source, target, send_sem, recv_sem, matrix, block, away):
        return pltpu.make_async_remote_copy(
            src_ref=source.at[order.index((matrix, rank_of(block)))],
            dst_ref=target.at[matrix, block],
            send_sem=send_sem.at[matrix, block],
            recv_sem=recv_sem.at[matrix, block],
            device_id={"dp": (me + group + 4 * away) % group},
            device_id_type=MESH,
        )

    def up_copy(matrix, block):
        return row_copy(side_out, low_in, low_send, low_recv, matrix, block, 1)

    def down_copy(matrix, block):
        return row_copy(side_out, high_in, high_send, high_recv, matrix, block, -1)

    def deep_up(matrix, block):
        return row_copy(deep_s, deep_low, rise_send, rise_recv, matrix, block, 1)

    def deep_down(matrix, block):
        return row_copy(deep_s, deep_high, down_send, down_recv, matrix, block, -1)

    def cross_copy(matrix):
        return pltpu.make_async_remote_copy(
            src_ref=cross_out.at[matrix],
            dst_ref=cross_in.at[matrix],
            send_sem=cross_send.at[matrix],
            recv_sem=cross_recv.at[matrix],
            device_id={"dp": me + 2 - 4 * side},
            device_id_type=MESH,
        )

    outs = (proj_out, value_out)

    def core_sum(turn, index, part, lanes):
        mine = kept_s[turn, index, part, lanes].astype(jnp.float32)
        return mine + core_in[turn, index, part, lanes].astype(jnp.float32)

    def send_side(index):
        core_copy(0, index).wait_recv()

        def add(part):
            side_out[index, part] = core_sum(0, index, part, near_lanes).astype(jnp.bfloat16)
            deep_s[index, 0, part] = core_sum(0, index, part, deep_lanes).astype(jnp.bfloat16)

        over_block(add)
        side_copy(index).start()
        core_copy(1, index).wait_recv()

        def add_own(part):
            deep_s[index, 1, part] = core_sum(1, index, part, deep_lanes).astype(jnp.bfloat16)

        over_block(add_own)

    def terms_of(spot, matrix, block, up, down, low, high):
        terms = []
        if block >= spot and spot > 0:
            up(matrix, block).wait_recv()
            terms.append(low)
        if block <= spot and spot < far - 1:
            down(matrix, block).wait_recv()
            terms.append(high)
        return terms

    def deep_chain(spot, index):
        spot_now[0] = spot
        matrix, rank = order[index]
        block = ranks[spot][rank]
        terms = terms_of(spot, matrix, block, deep_up, deep_down, deep_low, deep_high)

        def add(part):
            for which in range(2):
                mine = deep_s[index, which, part].astype(jnp.float32)
                for term in terms:
                    mine = mine + term[matrix, block, which, part].astype(jnp.float32)
                if block != spot:
                    deep_s[index, which, part] = mine.astype(jnp.bfloat16)
                elif which == 0:
                    cross_out[matrix, part] = mine.astype(jnp.bfloat16)
                else:
                    outs[matrix][part, deep_lanes] = mine

        if terms or block == spot:
            over_block(add)
        if block > spot:
            deep_up(matrix, block).start()
        elif block < spot:
            deep_down(matrix, block).start()
        else:
            cross_copy(matrix).start()

    def chain(spot, index):
        spot_now[0] = spot
        matrix, rank = order[index]
        block = ranks[spot][rank]
        side_copy(index).wait_send()
        side_copy(index).wait_recv()
        terms = terms_of(spot, matrix, block, up_copy, down_copy, low_in, high_in)

        def add(part):
            mine = core_sum(1, index, part, near_lanes)
            mine = mine + side_in[index, part].astype(jnp.float32)
            for term in terms:
                mine = mine + term[matrix, block, part].astype(jnp.float32)
            if block == spot:
                outs[matrix][part, near_lanes] = mine
            else:
                side_out[index, part] = mine.astype(jnp.bfloat16)

        over_block(add)
        if block > spot:
            up_copy(matrix, block).start()
        elif block < spot:
            down_copy(matrix, block).start()

    def at_spots(spots, body):
        for spot in spots:
            @pl.when(place == spot)
            def run(spot=spot):
                body(spot)

    ends = sorted({0, far - 1})

    def early(index):
        send_side(index)
        if order[index][1] < far - 1:
            at_spots(ends, lambda spot: deep_chain(spot, index))

    for index in range(pieces):
        if order[index] == (1, 0) or (far == 1 and index == 1):
            @pl.when(section == 0)
            def values_last():
                to_values(unit_rows_at(units - 1))

        for turn in range(2):
            partial(turn, index)
            core_copy(turn, index).start()
        if index > 0:
            early(index - 1)
    early(pieces - 1)

    def pass_deep(spot):
        for index in range(pieces):
            if order[index][1] < far - 1:
                deep_chain(spot, index)

    def own_deep(spot):
        for index in range(pieces):
            if order[index][1] == far - 1:
                deep_chain(spot, index)

    at_spots([spot for spot in range(far) if spot not in ends], pass_deep)

    def finish(spot):
        spot_now[0] = spot
        for matrix in range(2):
            for block in range(far):
                if block > spot:
                    up_copy(matrix, block).wait_send()
                    deep_up(matrix, block).wait_send()
                elif block < spot:
                    down_copy(matrix, block).wait_send()
                    deep_down(matrix, block).wait_send()

    def stage(indices):
        def body(spot):
            for index in indices:
                chain(spot, index)

        at_spots(range(far), body)

    ahead = min(units, pieces - 1)
    for index in range(ahead):
        stage([index])
        if index == min(OWN_DEEP, ahead - 1):
            at_spots(range(far), own_deep)

        @pl.when(section == 0)
        def tables(index=index):
            for unit in range(index, units if index == ahead - 1 else index + 1):
                table_rows(unit)

    lanes = table_out.shape[2]
    table = jnp.concatenate(
        [jnp.sum(tab_s[index], axis=0, keepdims=True) for index in range(3)]
        + [jnp.zeros((5, width), jnp.float32)], axis=0,
    )
    for owner in range(group):
        tables_s[owner, :, :lanes] = table[:, owner * lanes:(owner + 1) * lanes]

    def table_copy(step):
        return pltpu.make_async_remote_copy(
            src_ref=tables_s.at[(me + step) % group],
            dst_ref=tables_in.at[step - 1],
            send_sem=table_send.at[step - 1],
            recv_sem=table_recv.at[step - 1],
            device_id={"dp": (me + step) % group},
            device_id_type=MESH,
        )

    for step in range(1, group):
        table_copy(step).start()
    stage(range(ahead, pieces))
    sums = tables_s[me]
    for step in range(1, group):
        table_copy(step).wait_recv()
        sums = sums + tables_in[step - 1]
    for matrix in range(2):
        cross_copy(matrix).wait_recv()

        def add_cross(part):
            outs[matrix][part, deep_lanes] += cross_in[matrix, part].astype(jnp.float32)

        over_block(add_cross)
    for index in range(3):
        table_out[index] = sums[index:index + 1, :lanes]

    @pl.loop(0, hops)
    def sent(index):
        hop(index).wait_send()

    for index in range(pieces):
        core_copy(0, index).wait_send()
        core_copy(1, index).wait_send()
    for matrix in range(2):
        cross_copy(matrix).wait_send()
    for step in range(1, group):
        table_copy(step).wait_send()
    at_spots(range(far), finish)


def place_kernel(value_ref, proj_ref, table_ref, value_out, proj_out, table_out):
    value_out[...] = value_ref[...]
    proj_out[...] = proj_ref[...]
    table_out[...] = table_ref[...]


def per_device(
    inputs, out_grad, guide_bin, time_step, guide_table, section_table, value_weight, proj_weight
):
    units, rows, width = inputs.shape
    depth = value_weight.shape[2]
    group = lax.axis_size("dp")
    per_sample = rows * group // guide_bin.shape[1]
    if (lax.axis_size("section") != 2 or group % 4 or per_sample % rows or rows % 128
            or width != depth or width % (group * 16) or width < 768):
        return per_device_scan(
            inputs, out_grad, guide_bin, time_step, guide_table, section_table,
            value_weight, proj_weight,
        )
    far = group // 4
    count = units * rows
    piece = math.gcd(rows, PIECE_ROWS)
    hops = count // piece
    block = (width // group, width)
    pieces = 2 * far
    deep = (block[0], width // 6 // 128 * 128)
    near = (block[0], width - deep[1])
    lanes = width // group
    vmem = pl.BlockSpec(memory_space=pltpu.VMEM)
    smem = pl.BlockSpec(memory_space=pltpu.SMEM)
    hbm = pl.BlockSpec(memory_space=pl.ANY)
    dma = pltpu.SemaphoreType.DMA
    half = jnp.bfloat16
    shapes = (
        jax.ShapeDtypeStruct(block, jnp.float32),
        jax.ShapeDtypeStruct(block, jnp.float32),
        jax.ShapeDtypeStruct((3, 1, lanes), jnp.float32),
    )
    sums = pl.pallas_call(
        functools.partial(step_kernel, far),
        out_shape=shapes,
        in_specs=[smem, smem, vmem, vmem, hbm, hbm, hbm, hbm],
        out_specs=(vmem,) * 3,
        scratch_shapes=[
            pltpu.VMEM((count, width), half),
            pltpu.VMEM((width, depth), half),
            pltpu.VMEM((depth, width), half),
            pltpu.VMEM((units, 3, 1, width), jnp.float32),
            pltpu.VMEM((count, width), half),
            pltpu.VMEM((count, width), half),
            pltpu.VMEM((count, width), half),
            pltpu.VMEM((count, depth), half),
            pltpu.VMEM((2, width, count), half),
            pltpu.VMEM((2, count, width), half),
            pltpu.VMEM((count, width), jnp.float32),
            pltpu.VMEM((rows, width), jnp.float32),
            pltpu.VMEM((3, 8, width), jnp.float32),
            pltpu.VMEM((2, pieces) + block, half),
            pltpu.VMEM((2, pieces) + block, half),
            pltpu.VMEM((2, pieces) + block, half),
            pltpu.VMEM((pieces,) + near, half),
            pltpu.VMEM((pieces,) + near, half),
            pltpu.VMEM((2, far) + near, half),
            pltpu.VMEM((2, far) + near, half),
            pltpu.VMEM((pieces, 2) + deep, half),
            pltpu.VMEM((2, far, 2) + deep, half),
            pltpu.VMEM((2, far, 2) + deep, half),
            pltpu.VMEM((2,) + deep, half),
            pltpu.VMEM((2,) + deep, half),
            pltpu.VMEM((group, 8, 128), jnp.float32),
            pltpu.VMEM((group - 1, 8, 128), jnp.float32),
            dma((2 + units,)), dma((hops,)), dma((hops,)), dma((2, pieces)), dma((2, pieces)),
            dma((pieces,)), dma((pieces,)), dma((2, far)), dma((2, far)), dma((2, far)),
            dma((2, far)), dma((2, far)), dma((2, far)), dma((2, far)), dma((2, far)),
            dma((2,)), dma((2,)), dma((group - 1,)), dma((group - 1,)),
        ],
        compiler_params=pltpu.CompilerParams(
            collective_id=0, has_side_effects=True, vmem_limit_bytes=62 * 1024 * 1024
        ),
    )(
        guide_bin.reshape(-1), time_step.reshape(-1), guide_table,
        section_table.transpose(1, 0, 2), inputs, out_grad,
        value_weight, proj_weight,
    )
    value_sum, proj_sum, table_sum = pl.pallas_call(
        place_kernel, out_shape=shapes, in_specs=[vmem] * 3, out_specs=(vmem,) * 3
    )(*sums)
    return (value_sum[None], proj_sum[None], table_sum.transpose(1, 0, 2))


def solution(mesh):
    return jax.shard_map(
        per_device,
        mesh=mesh,
        in_specs=(
            P(None, "dp", None),
            P(None, "dp", None),
            P(),
            P(),
            P(),
            P("section", None, None),
            P("section", None, None),
            P("section", None, None),
        ),
        out_specs=(P("section", "dp", None), P("section", "dp", None), P("section", None, "dp")),
        check_vma=False,
    )
```

```python
import functools
import math

import jax
import jax.numpy as jnp
from jax import lax
from jax.experimental import pallas as pl
from jax.experimental.pallas import tpu as pltpu
from jax.sharding import PartitionSpec as P

NORM_FLOOR = 0.1
PIECE_ROWS = 32
FORWARD_ROWS = 64
CHUNK_ROWS = 16
UNROLL = 2
TILE = 1536
OWN_DEEP = 2
TABLES_AHEAD = 1


def shifted(value, axis, steps):
    count = lax.axis_size(axis)
    leading, last = (max(0, -steps), min(count, count - steps))
    return lax.ppermute(value, axis, [(source, source + steps) for source in range(leading, last)])


def normalize(hidden):
    centre = jnp.mean(hidden, axis=-1, keepdims=True)
    centred = hidden - centre
    spread = jnp.mean(centred * centred, axis=-1, keepdims=True)
    inverse = lax.rsqrt(spread + NORM_FLOOR)
    return (centred * inverse, inverse)


def conditions(guide_bin, time_step, guide_table):
    total = guide_table.shape[1]
    half = total // 2
    frequency = jnp.exp(-math.log(10000.0) * jnp.arange(half, dtype=jnp.float32) / half)
    angle = time_step.astype(jnp.float32)[..., None] * frequency
    waves = jnp.concatenate([jnp.sin(angle), jnp.cos(angle)], axis=-1)
    bin_count = guide_table.shape[0]
    onehot = (guide_bin[..., None] == jnp.arange(bin_count, dtype=jnp.int32)).astype(jnp.float32)
    picked = jnp.einsum(
        "msb,bw->msw", onehot, guide_table.astype(jnp.float32), precision=lax.Precision.HIGHEST
    )
    return picked + 0.5 * waves


def contract_rows(left, right):
    return lax.dot_general(
        left, right, (((0,), (0,)), ((), ())), preferred_element_type=jnp.float32
    )


def forward_block(block_in, modulation, value_weight, proj_weight):
    width = block_in.shape[1]
    hidden = block_in.astype(jnp.float32)
    normed, inverse = normalize(hidden)
    shift = modulation[:, :width]
    scale = modulation[:, width : 2 * width]
    gate = modulation[:, 2 * width :]
    modulated = (normed * (1.0 + scale) + shift).astype(jnp.bfloat16)
    values = jnp.dot(modulated, value_weight, preferred_element_type=jnp.float32).astype(
        jnp.bfloat16
    )
    projected = jnp.dot(values, proj_weight, preferred_element_type=jnp.float32)
    block_out = (hidden + gate * projected).astype(jnp.bfloat16)
    return (block_out, modulated, values, projected)


def backward_block(block_in, projected, upstream, modulation, value_weight, proj_weight):
    width = block_in.shape[1]
    hidden = block_in.astype(jnp.float32)
    normed, inverse = normalize(hidden)
    scale = modulation[:, width : 2 * width]
    gate = modulation[:, 2 * width :]
    grad_up = upstream.astype(jnp.float32)
    grad_proj = (gate * grad_up).astype(jnp.bfloat16)
    grad_values = lax.dot_general(
        grad_proj, proj_weight, (((1,), (1,)), ((), ())), preferred_element_type=jnp.float32
    ).astype(jnp.bfloat16)
    grad_mod = lax.dot_general(
        grad_values, value_weight, (((1,), (1,)), ((), ())), preferred_element_type=jnp.float32
    )
    part_table = jnp.stack(
        [
            jnp.sum(grad_mod, axis=0),
            jnp.sum(grad_mod * normed, axis=0),
            jnp.sum(grad_up * projected, axis=0),
        ]
    )
    grad_norm = grad_mod * (1.0 + scale)
    centre_grad = jnp.mean(grad_norm, axis=-1, keepdims=True)
    cross = jnp.mean(grad_norm * normed, axis=-1, keepdims=True)
    grad_in = grad_up + inverse * (grad_norm - centre_grad - normed * cross)
    return (grad_in.astype(jnp.bfloat16), grad_values, grad_proj, part_table)


def per_device_scan(
    inputs, out_grad, guide_bin, time_step, guide_table, section_table, value_weight, proj_weight
):
    sections = lax.axis_size("section")
    section_id = lax.axis_index("section")
    position = lax.axis_index("dp")
    group_size = lax.axis_size("dp")
    tok_dev = inputs.shape[1]
    width = inputs.shape[2]
    value_width = value_weight.shape[2]
    batches = inputs.shape[0]
    samples = guide_bin.shape[1]
    tokens = tok_dev * group_size
    rows_per = tokens // samples
    parts = 1
    unit_rows = tok_dev // parts
    units = batches * parts
    condition = conditions(guide_bin, time_step, guide_table)
    weights_value = value_weight[0]
    weights_proj = proj_weight[0]
    section_row = section_table[0].reshape(-1)
    sample_ids = jnp.arange(samples, dtype=jnp.int32)

    def unit_modulation(unit_id):
        batch_id = unit_id // parts
        piece_id = unit_id % parts
        chosen = lax.dynamic_index_in_dim(condition, batch_id, 0, keepdims=False)
        global_rows = (
            position * tok_dev + piece_id * unit_rows + jnp.arange(unit_rows, dtype=jnp.int32)
        )
        owner = global_rows // rows_per
        onehot = (owner[:, None] == sample_ids[None, :]).astype(jnp.float32)
        picked = jnp.dot(
            onehot, chosen, precision=lax.Precision.HIGHEST, preferred_element_type=jnp.float32
        )
        return picked + section_row

    slots = units + 1
    keep_in = jnp.zeros((slots, unit_rows, width), jnp.bfloat16)
    keep_mod = jnp.zeros((slots, unit_rows, width), jnp.bfloat16)
    keep_val = jnp.zeros((slots, unit_rows, value_width), jnp.bfloat16)
    keep_proj = jnp.zeros((slots, unit_rows, width), jnp.float32)
    arriving = jnp.zeros((unit_rows, width), jnp.bfloat16)

    def forward_tick(carry, tick_id):
        incoming, saved_in, saved_mod, saved_val, saved_proj = carry
        unit_id = tick_id - section_id
        valid = (unit_id >= 0) & (unit_id < units)
        clipped = jnp.clip(unit_id, 0, units - 1)
        first = lax.dynamic_index_in_dim(inputs, clipped, 0, keepdims=False)
        block_in = jnp.where(section_id == 0, first, incoming)

        def forward_active(operand):
            return forward_block(operand, unit_modulation(clipped), weights_value, weights_proj)

        def forward_resting(operand):
            return (
                jnp.zeros_like(operand),
                jnp.zeros_like(operand),
                jnp.zeros((unit_rows, value_width), jnp.bfloat16),
                jnp.zeros((unit_rows, width), jnp.float32),
            )

        block_out, modulated, values, projected = lax.cond(
            valid, forward_active, forward_resting, block_in
        )
        slot_id = jnp.where(valid, unit_id, units)
        saved_in = lax.dynamic_update_index_in_dim(saved_in, block_in, slot_id, 0)
        saved_mod = lax.dynamic_update_index_in_dim(saved_mod, modulated, slot_id, 0)
        saved_val = lax.dynamic_update_index_in_dim(saved_val, values, slot_id, 0)
        saved_proj = lax.dynamic_update_index_in_dim(saved_proj, projected, slot_id, 0)
        sent = shifted(block_out, "section", 1)
        return ((sent, saved_in, saved_mod, saved_val, saved_proj), None)

    ticks = jnp.arange(units + sections - 1, dtype=jnp.int32)
    carry, unused = lax.scan(
        forward_tick, (arriving, keep_in, keep_mod, keep_val, keep_proj), ticks
    )
    arriving, keep_in, keep_mod, keep_val, keep_proj = carry
    store = jnp.zeros((slots, unit_rows, value_width), jnp.bfloat16)
    extra_zero = jnp.zeros((unit_rows, value_width), jnp.bfloat16)
    keep_grad = jnp.zeros((slots, unit_rows, width), jnp.bfloat16)
    proj_sum = jnp.zeros((value_width, width), jnp.float32)
    table_sum = jnp.zeros((3, width), jnp.float32)

    def backward_tick(carry, tick_id):
        incoming, store_now, grads_now, proj_now, table_now = carry
        unit_id = tick_id - (sections - 1 - section_id)
        valid = (unit_id >= 0) & (unit_id < units)
        clipped = jnp.clip(unit_id, 0, units - 1)
        last = lax.dynamic_index_in_dim(out_grad, clipped, 0, keepdims=False)
        upstream = jnp.where(section_id == sections - 1, last, incoming)
        block_in = lax.dynamic_index_in_dim(keep_in, clipped, 0, keepdims=False)
        modulated = lax.dynamic_index_in_dim(keep_mod, clipped, 0, keepdims=False)
        values = lax.dynamic_index_in_dim(keep_val, clipped, 0, keepdims=False)
        projected = lax.dynamic_index_in_dim(keep_proj, clipped, 0, keepdims=False)

        def backward_active(operand):
            grad_in, grad_values, grad_proj, part_table = backward_block(
                block_in, projected, operand, unit_modulation(clipped), weights_value, weights_proj
            )
            part_proj = jnp.zeros((value_width, width), jnp.float32)
            return (grad_in, grad_values, grad_proj, part_proj, part_table)

        def backward_resting(operand):
            return (
                jnp.zeros_like(operand),
                extra_zero,
                jnp.zeros((unit_rows, width), jnp.bfloat16),
                jnp.zeros((value_width, width), jnp.float32),
                jnp.zeros((3, width), jnp.float32),
            )

        grad_in, extra, grad_proj, part_proj, part_table = lax.cond(
            valid, backward_active, backward_resting, upstream
        )
        slot_id = jnp.where(valid, unit_id, units)
        store_now = lax.dynamic_update_index_in_dim(store_now, extra, slot_id, 0)
        grads_now = lax.dynamic_update_index_in_dim(grads_now, grad_proj, slot_id, 0)
        sent = shifted(grad_in, "section", -1)
        return ((sent, store_now, grads_now, proj_now + part_proj, table_now + part_table), None)

    carry, unused = lax.scan(
        backward_tick, (arriving, store, keep_grad, proj_sum, table_sum), ticks
    )
    arriving, store, keep_grad, proj_sum, table_sum = carry
    mod_rows = keep_mod[:units].reshape(units * unit_rows, width)
    grad_rows = store[:units].reshape(units * unit_rows, value_width)
    columns = mod_rows
    value_part = lax.psum_scatter(
        contract_rows(columns, grad_rows), "dp", scatter_dimension=0, tiled=True
    )
    val_rows = keep_val[:units].reshape(units * unit_rows, value_width)
    upper_rows = keep_grad[:units].reshape(units * unit_rows, width)
    columns = val_rows
    proj_part = lax.psum_scatter(
        contract_rows(columns, upper_rows), "dp", scatter_dimension=0, tiled=True
    )
    table_part = lax.psum_scatter(table_sum, "dp", scatter_dimension=1, tiled=True)
    return (value_part[None], proj_part[None], table_part[None])


MESH = pl.DeviceIdType.MESH


def step_kernel(far, bin_ref, time_ref, guide_hbm, section_ref, x_hbm, up_hbm, wv_hbm, wp_hbm,
                value_out, proj_out, table_out, guide_ref,
                local_s, wv_s, wp_s, rows_s, arrive_s, send_s, mod_s, val_s, left_s, right_s,
                wide_s, part_s, tab_s, made_s, core_in, side_out, side_in, low_in, high_in,
                deep_s, deep_low, deep_high, cross_out, cross_in,
                tables_s, tables_in, small_sem, load_sem, hop_send, hop_recv, core_send, core_recv,
                side_send, side_recv, low_send, low_recv, high_send, high_recv,
                down_send, down_recv, rise_send, rise_recv, cross_send, cross_recv,
                table_send, table_recv):
    units, unit_rows = x_hbm.shape[0], x_hbm.shape[1]
    count, width = local_s.shape
    depth = wv_s.shape[1]
    hops = hop_send.shape[0]
    piece = count // hops
    per_unit = unit_rows // piece
    group = 4 * far
    section = lax.axis_index("section")
    me = lax.axis_index("dp")
    core, side, place = me % 2, (me // 2) % 2, me // 4

    load_guide = pltpu.make_async_copy(guide_hbm, guide_ref, small_sem.at[0])
    load_guide.start()

    def load_rows(source, unit):
        part = pl.ds(unit * unit_rows, unit_rows)
        return pltpu.make_async_copy(source.at[unit], local_s.at[part], load_sem.at[2 + unit])

    load_value = pltpu.make_async_copy(wv_hbm.at[0], wv_s, load_sem.at[0])
    load_proj = pltpu.make_async_copy(wp_hbm.at[0], wp_s, load_sem.at[1])

    @pl.when(section == 0)
    def load_first():
        load_rows(x_hbm, 0).start()
        load_value.start()
        load_proj.start()
        for unit in range(1, units):
            load_rows(x_hbm, unit).start()

    @pl.when(section == 1)
    def load_last():
        load_rows(up_hbm, 0).start()
        load_proj.start()
        load_value.start()
        for unit in range(1, units):
            load_rows(up_hbm, unit).start()

    barrier = pltpu.get_barrier_semaphore()
    pl.semaphore_signal(
        barrier, inc=1, device_id={"section": 1 - section}, device_id_type=MESH
    )
    for step in range(1, group):
        pl.semaphore_signal(
            barrier, inc=1, device_id={"dp": (me + step) % group}, device_id_type=MESH
        )

    load_guide.wait()
    total = guide_ref.shape[1]
    half = total // 2
    samples = bin_ref.shape[0] // units
    sample = (me * unit_rows) // (unit_rows * group // samples)
    lane = lax.broadcasted_iota(jnp.int32, (units, half), 1).astype(jnp.float32)
    frequency = jnp.exp(-math.log(10000.0) * lane / half)
    which = lax.broadcasted_iota(jnp.int32, (units, half), 0)
    times = jnp.zeros((units, half), jnp.float32)
    for unit in range(units):
        time = time_ref[unit * samples + sample].astype(jnp.float32)
        times = jnp.where(which == unit, time, times)
    angle = times * frequency
    waves = jnp.concatenate([jnp.sin(angle), jnp.cos(angle)], axis=1)
    table = guide_ref[...].astype(jnp.float32)
    bins = lax.broadcasted_iota(jnp.int32, table.shape, 0)
    for unit in range(units):
        picked = jnp.sum(
            jnp.where(bins == bin_ref[unit * samples + sample], table, 0.0),
            axis=0, keepdims=True,
        )
        picked = picked + 0.5 * waves[unit:unit + 1]
        for index in range(3):
            lanes = slice(index * width, (index + 1) * width)
            rows_s[unit, index] = picked[:, lanes] + section_ref[index]
    tab_s[...] = jnp.zeros_like(tab_s)

    def hop(index):
        part = pl.ds(pl.multiple_of(index * piece, piece), piece)
        return pltpu.make_async_remote_copy(
            src_ref=send_s.at[part],
            dst_ref=arrive_s.at[part],
            send_sem=hop_send.at[index],
            recv_sem=hop_recv.at[index],
            device_id={"section": 1 - section},
            device_id_type=MESH,
        )

    def each_chunk(start, size, body):
        tall = math.gcd(size, CHUNK_ROWS)

        @pl.loop(0, size // tall, unroll=min(UNROLL, size // tall))
        def step(index):
            body(pl.ds(pl.multiple_of(start + index * tall, tall), tall), index * tall)

    def multiply(size, body):
        tile = math.gcd(size, TILE)

        @pl.loop(0, size // tile)
        def step(index):
            body(pl.ds(pl.multiple_of(index * tile, tile), tile))

    def add_rows(index, value):
        rows = value.shape[0]
        tab_s[index] += jnp.sum(value.reshape(rows // 8, 8, width), axis=0)

    def to_depth(rows, part):
        val_s[rows, part] = jnp.dot(
            mod_s[rows], wv_s[:, part], preferred_element_type=jnp.float32
        ).astype(jnp.bfloat16)

    def to_width(rows, part):
        return jnp.dot(val_s[rows], wp_s[:, part], preferred_element_type=jnp.float32)

    def to_values(rows):
        def body(part):
            right_s[1, rows, part] = lax.dot_general(
                right_s[0, rows], wp_s[part, :], (((1,), (1,)), ((), ())),
                preferred_element_type=jnp.float32,
            ).astype(jnp.bfloat16)

        multiply(depth, body)

    def to_mod(rows, target, target_rows):
        def body(part):
            target[target_rows, part] = lax.dot_general(
                right_s[1, rows], wv_s[part, :], (((1,), (1,)), ((), ())),
                preferred_element_type=jnp.float32,
            )

        multiply(width, body)

    def unit_rows_at(unit):
        return pl.ds(pl.multiple_of(unit * unit_rows, unit_rows), unit_rows)

    def turn_left(unit):
        part = unit_rows_at(unit)
        left_s[0, :, part] = val_s[part].T
        left_s[1, :, part] = mod_s[part].T

    def forward(index, size):
        start = pl.multiple_of(index * size, size)
        unit = start // unit_rows
        rows = pl.ds(start, size)

        def modulate(part, unused):
            normed, inverse = normalize(local_s[part].astype(jnp.float32))
            scaled = normed * (1.0 + rows_s[unit, 1]) + rows_s[unit, 0]
            mod_s[part] = scaled.astype(jnp.bfloat16)

        each_chunk(start, size, modulate)
        multiply(depth, lambda part: to_depth(rows, part))

        @pl.when(index == 0)
        def load_second():
            load_proj.wait()

        def second(part):
            wide_s[rows, part] = to_width(rows, part)

        multiply(width, second)

        @pl.when(index == 0)
        def enter():
            for unit in range(1, units):
                load_rows(x_hbm, unit).wait()
            pl.semaphore_wait(barrier, group)

        def add_gated(part, unused):
            hidden = local_s[part].astype(jnp.float32)
            block_out = hidden + rows_s[unit, 2] * wide_s[part]
            send_s[part] = block_out.astype(jnp.bfloat16)

        for at in range(size // piece):
            each_chunk(start + at * piece, piece, add_gated)
            hop(index * (size // piece) + at).start()

    def receive(index):
        start = pl.multiple_of(index * piece, piece)
        unit = start // unit_rows
        hop(index).wait_recv()

        def body(part, unused):
            grad_up = arrive_s[part].astype(jnp.float32)
            right_s[0, part] = (rows_s[unit, 2] * grad_up).astype(jnp.bfloat16)
            add_rows(2, grad_up * wide_s[part])

        each_chunk(start, piece, body)

    def table_rows(unit):
        to_mod(unit_rows_at(unit), part_s, slice(None))

        def body(part, offset):
            normed, inverse = normalize(local_s[part].astype(jnp.float32))
            grad_mod = part_s[pl.ds(offset, part.size)]
            add_rows(0, grad_mod)
            add_rows(1, grad_mod * normed)

        each_chunk(unit * unit_rows, unit_rows, body)

    @pl.when(section == 0)
    def earlier():
        load_rows(x_hbm, 0).wait()
        load_value.wait()
        size = math.gcd(unit_rows, FORWARD_ROWS)

        @pl.loop(0, units)
        def out(unit):
            @pl.loop(0, unit_rows // size)
            def some(at):
                forward(unit * (unit_rows // size) + at, size)

            turn_left(unit)

        @pl.loop(0, units)
        def back(unit):
            @pl.loop(0, per_unit)
            def one(at):
                receive(unit * per_unit + at)

            @pl.when(unit < units - 1)
            def values_now():
                to_values(unit_rows_at(unit))

            @pl.when(unit < min(TABLES_AHEAD, units - 1))
            def tables_now():
                table_rows(unit)

    def grads_ahead(unit):
        def body(part, unused):
            grad_up = local_s[part].astype(jnp.float32)
            right_s[0, part] = (rows_s[unit, 2] * grad_up).astype(jnp.bfloat16)

        each_chunk(unit * unit_rows, unit_rows, body)
        to_values(unit_rows_at(unit))

    def mods_ahead(unit):
        rows = unit_rows_at(unit)
        to_mod(rows, wide_s, rows)

    def values_behind(unit):
        multiply(depth, lambda part: to_depth(unit_rows_at(unit), part))

    def gates_behind(unit):
        rows = unit_rows_at(unit)

        def second(part):
            part_s[:, part] = to_width(rows, part)

        multiply(width, second)

        def body(part, offset):
            add_rows(2, local_s[part].astype(jnp.float32) * part_s[pl.ds(offset, part.size)])

        each_chunk(unit * unit_rows, unit_rows, body)

    def answer(index):
        start = pl.multiple_of(index * piece, piece)
        unit = start // unit_rows
        hop(index).wait_recv()

        def body(part, unused):
            normed, inverse = normalize(arrive_s[part].astype(jnp.float32))
            scale = 1.0 + rows_s[unit, 1]
            mod_s[part] = (normed * scale + rows_s[unit, 0]).astype(jnp.bfloat16)
            grad_mod = wide_s[part]
            add_rows(0, grad_mod)
            add_rows(1, grad_mod * normed)
            grad_norm = grad_mod * scale
            centre_grad = jnp.mean(grad_norm, axis=-1, keepdims=True)
            cross = jnp.mean(grad_norm * normed, axis=-1, keepdims=True)
            grad_up = local_s[part].astype(jnp.float32)
            grad_in = grad_up + inverse * (grad_norm - centre_grad - normed * cross)
            send_s[part] = grad_in.astype(jnp.bfloat16)

        each_chunk(start, piece, body)
        hop(index).start()

    @pl.when(section == 1)
    def later():
        load_rows(up_hbm, 0).wait()
        load_proj.wait()
        load_value.wait()
        for unit in range(1, units):
            load_rows(up_hbm, unit).wait()
        for unit in range(min(2, units)):
            grads_ahead(unit)
            mods_ahead(unit)
        pl.semaphore_wait(barrier, group)

        @pl.loop(0, units)
        def both(unit):
            @pl.loop(0, per_unit)
            def one(at):
                answer(unit * per_unit + at)

                @pl.when((at == 0) & (unit + 2 < units))
                def job_grads():
                    grads_ahead(unit + 2)

                @pl.when((at == 1) & (unit + 2 < units))
                def job_mods():
                    mods_ahead(unit + 2)

                @pl.when((at == 2 % per_unit) & (unit >= 1))
                def job_values():
                    values_behind(unit - 1)
                    turn_left(unit - 1)

                @pl.when((at == 3 % per_unit) & (unit >= 1) & (unit < units - 1))
                def job_gates():
                    gates_behind(unit - 1)

        values_behind(units - 1)
        turn_left(units - 1)

    ranks = [sorted(range(far), key=lambda block: -abs(block - spot)) for spot in range(far)]
    order = [(matrix, rank) for rank in range(far - 1) for matrix in range(2)]
    order = order + [(0, far - 1), (1, far - 1)]
    pieces = len(order)
    block_rows = left_s.shape[1] // group
    per_matrix = far - 1

    def chosen(values):
        result = 0
        for spot in range(far):
            away = (place - spot + far) % far
            result = result + values[spot] * (1 - (away + far - 1) // far)
        return result

    blocks = [chosen([ranks[spot][rank] for spot in range(far)]) for rank in range(far)]

    def partial(turn, index):
        matrix, rank = order[index]
        which = (1 - side) if turn == 0 else side
        first = pl.multiple_of((blocks[rank] * 2 + which) * 2 * block_rows, 2 * block_rows)
        product = jnp.dot(
            left_s[matrix, pl.ds(first, 2 * block_rows)], right_s[matrix],
            preferred_element_type=jnp.float32,
        )
        made_s[turn, index] = product.astype(jnp.bfloat16).reshape(2, block_rows, width)

    def core_copy(turn, index):
        return pltpu.make_async_remote_copy(
            src_ref=made_s.at[turn, index, 1 - core],
            dst_ref=core_in.at[turn, index],
            send_sem=core_send.at[turn, index],
            recv_sem=core_recv.at[turn, index],
            device_id={"dp": me + 1 - 2 * core},
            device_id_type=MESH,
        )

    def side_copy(index):
        return pltpu.make_async_remote_copy(
            src_ref=side_out.at[index],
            dst_ref=side_in.at[index],
            send_sem=side_send.at[index],
            recv_sem=side_recv.at[index],
            device_id={"dp": me + 2 - 4 * side},
            device_id_type=MESH,
        )

    def over_block(body):
        tall = math.gcd(block_rows, 16)

        @pl.loop(0, block_rows // tall)
        def step(at):
            body(pl.ds(pl.multiple_of(at * tall, tall), tall))

    near = side_out.shape[2]
    near_lanes, deep_lanes = slice(0, near), slice(near, width)
    spot_now = [0]

    def rank_of(block):
        return ranks[spot_now[0]].index(block)

    def row_copy(source, target, send_sem, recv_sem, matrix, block, away):
        return pltpu.make_async_remote_copy(
            src_ref=source.at[order.index((matrix, rank_of(block)))],
            dst_ref=target.at[matrix, block],
            send_sem=send_sem.at[matrix, block],
            recv_sem=recv_sem.at[matrix, block],
            device_id={"dp": (me + group + 4 * away) % group},
            device_id_type=MESH,
        )

    def up_copy(matrix, block):
        return row_copy(side_out, low_in, low_send, low_recv, matrix, block, 1)

    def down_copy(matrix, block):
        return row_copy(side_out, high_in, high_send, high_recv, matrix, block, -1)

    def deep_up(matrix, block):
        return row_copy(deep_s, deep_low, rise_send, rise_recv, matrix, block, 1)

    def deep_down(matrix, block):
        return row_copy(deep_s, deep_high, down_send, down_recv, matrix, block, -1)

    def cross_copy(matrix):
        return pltpu.make_async_remote_copy(
            src_ref=cross_out.at[matrix],
            dst_ref=cross_in.at[matrix],
            send_sem=cross_send.at[matrix],
            recv_sem=cross_recv.at[matrix],
            device_id={"dp": me + 2 - 4 * side},
            device_id_type=MESH,
        )

    outs = (proj_out, value_out)

    def core_sum(turn, index, part, lanes):
        mine = made_s[turn, index, core, part, lanes].astype(jnp.float32)
        return mine + core_in[turn, index, part, lanes].astype(jnp.float32)

    def send_side(index):
        core_copy(0, index).wait_recv()

        def add(part):
            side_out[index, part] = core_sum(0, index, part, near_lanes).astype(jnp.bfloat16)
            deep_s[index, 0, part] = core_sum(0, index, part, deep_lanes).astype(jnp.bfloat16)

        over_block(add)
        side_copy(index).start()
        core_copy(1, index).wait_recv()

        def add_own(part):
            deep_s[index, 1, part] = core_sum(1, index, part, deep_lanes).astype(jnp.bfloat16)

        over_block(add_own)

    def terms_of(spot, matrix, block, up, down, low, high):
        terms = []
        if block >= spot and spot > 0:
            up(matrix, block).wait_recv()
            terms.append(low)
        if block <= spot and spot < far - 1:
            down(matrix, block).wait_recv()
            terms.append(high)
        return terms

    def deep_chain(spot, index):
        spot_now[0] = spot
        matrix, rank = order[index]
        block = ranks[spot][rank]
        terms = terms_of(spot, matrix, block, deep_up, deep_down, deep_low, deep_high)

        def add(part):
            for which in range(2):
                mine = deep_s[index, which, part].astype(jnp.float32)
                for term in terms:
                    mine = mine + term[matrix, block, which, part].astype(jnp.float32)
                if block != spot:
                    deep_s[index, which, part] = mine.astype(jnp.bfloat16)
                elif which == 0:
                    cross_out[matrix, part] = mine.astype(jnp.bfloat16)
                else:
                    outs[matrix][part, deep_lanes] = mine

        if terms or block == spot:
            over_block(add)
        if block > spot:
            deep_up(matrix, block).start()
        elif block < spot:
            deep_down(matrix, block).start()
        else:
            cross_copy(matrix).start()

    def chain(spot, index):
        spot_now[0] = spot
        matrix, rank = order[index]
        block = ranks[spot][rank]
        side_copy(index).wait_send()
        side_copy(index).wait_recv()
        terms = terms_of(spot, matrix, block, up_copy, down_copy, low_in, high_in)

        def add(part):
            mine = core_sum(1, index, part, near_lanes)
            mine = mine + side_in[index, part].astype(jnp.float32)
            for term in terms:
                mine = mine + term[matrix, block, part].astype(jnp.float32)
            if block == spot:
                outs[matrix][part, near_lanes] = mine
            else:
                side_out[index, part] = mine.astype(jnp.bfloat16)

        over_block(add)
        if block > spot:
            up_copy(matrix, block).start()
        elif block < spot:
            down_copy(matrix, block).start()

    def at_spots(spots, body):
        for spot in spots:
            @pl.when(place == spot)
            def run(spot=spot):
                body(spot)

    ends = sorted({0, far - 1})

    def early(index):
        send_side(index)
        if order[index][1] < far - 1:
            at_spots(ends, lambda spot: deep_chain(spot, index))

    for index in range(pieces):
        if index == 1:
            @pl.when(section == 0)
            def values_last():
                to_values(unit_rows_at(units - 1))

        for turn in range(2):
            partial(turn, index)
            core_copy(turn, index).start()
        if index > 0:
            early(index - 1)
    early(pieces - 1)

    def pass_deep(spot):
        for index in range(pieces):
            if order[index][1] < far - 1:
                deep_chain(spot, index)

    def own_deep(spot):
        for index in range(pieces):
            if order[index][1] == far - 1:
                deep_chain(spot, index)

    at_spots([spot for spot in range(far) if spot not in ends], pass_deep)

    def finish(spot):
        spot_now[0] = spot
        for matrix in range(2):
            for block in range(far):
                if block > spot:
                    up_copy(matrix, block).wait_send()
                    deep_up(matrix, block).wait_send()
                elif block < spot:
                    down_copy(matrix, block).wait_send()
                    deep_down(matrix, block).wait_send()

    def stage(indices):
        def body(spot):
            for index in indices:
                chain(spot, index)

        at_spots(range(far), body)

    ahead = min(units, pieces - 1)
    for index in range(ahead):
        stage([index])
        if index == min(OWN_DEEP, ahead - 1):
            at_spots(range(far), own_deep)

        last = index == ahead - 1
        behind = (index + TABLES_AHEAD) % units
        spare = [behind] if ahead == units else range(index, units if last else index + 1)

        @pl.when(section == 0)
        def tables(spare=spare):
            for unit in spare:
                if unit >= min(TABLES_AHEAD, units - 1):
                    table_rows(unit)

        @pl.when(section == 1)
        def gates(index=index):
            if index < min(2, units):
                gates_behind(units - 1 - index)

    lanes = table_out.shape[2]
    table = jnp.concatenate(
        [jnp.sum(tab_s[index], axis=0, keepdims=True) for index in range(3)]
        + [jnp.zeros((5, width), jnp.float32)], axis=0,
    )
    for owner in range(group):
        tables_s[owner, :, :lanes] = table[:, owner * lanes:(owner + 1) * lanes]

    def table_copy(step):
        return pltpu.make_async_remote_copy(
            src_ref=tables_s.at[(me + step) % group],
            dst_ref=tables_in.at[step - 1],
            send_sem=table_send.at[step - 1],
            recv_sem=table_recv.at[step - 1],
            device_id={"dp": (me + step) % group},
            device_id_type=MESH,
        )

    for step in range(1, group):
        table_copy(step).start()
    stage(range(ahead, pieces - 2))
    sums = tables_s[me]
    for step in range(1, group):
        table_copy(step).wait_recv()
        sums = sums + tables_in[step - 1]
    for row in range(3):
        table_out[row] = sums[row:row + 1, :lanes]
    stage(range(max(ahead, pieces - 2), pieces))
    for matrix in range(2):
        cross_copy(matrix).wait_recv()

        def add_cross(part):
            outs[matrix][part, deep_lanes] += cross_in[matrix, part].astype(jnp.float32)

        over_block(add_cross)

    @pl.loop(0, hops)
    def sent(index):
        hop(index).wait_send()

    for index in range(pieces):
        core_copy(0, index).wait_send()
        core_copy(1, index).wait_send()
    for matrix in range(2):
        cross_copy(matrix).wait_send()
    for step in range(1, group):
        table_copy(step).wait_send()
    at_spots(range(far), finish)


def place_kernel(value_ref, proj_ref, table_ref, value_out, proj_out, table_out):
    value_out[...] = value_ref[...]
    proj_out[...] = proj_ref[...]
    table_out[...] = table_ref[...]


def per_device(
    inputs, out_grad, guide_bin, time_step, guide_table, section_table, value_weight, proj_weight
):
    units, rows, width = inputs.shape
    depth = value_weight.shape[2]
    group = lax.axis_size("dp")
    per_sample = rows * group // guide_bin.shape[1]
    if (lax.axis_size("section") != 2 or group % 4 or per_sample % rows or rows % 128
            or width != depth or width % (group * 16) or width < 768):
        return per_device_scan(
            inputs, out_grad, guide_bin, time_step, guide_table, section_table,
            value_weight, proj_weight,
        )
    far = group // 4
    count = units * rows
    piece = math.gcd(rows, PIECE_ROWS)
    hops = count // piece
    block = (width // group, width)
    pieces = 2 * far
    deep = (block[0], width // 6 // 128 * 128)
    near = (block[0], width - deep[1])
    lanes = width // group
    vmem = pl.BlockSpec(memory_space=pltpu.VMEM)
    smem = pl.BlockSpec(memory_space=pltpu.SMEM)
    hbm = pl.BlockSpec(memory_space=pl.ANY)
    dma = pltpu.SemaphoreType.DMA
    half = jnp.bfloat16
    shapes = (
        jax.ShapeDtypeStruct(block, jnp.float32),
        jax.ShapeDtypeStruct(block, jnp.float32),
        jax.ShapeDtypeStruct((3, 1, lanes), jnp.float32),
    )
    sums = pl.pallas_call(
        functools.partial(step_kernel, far),
        out_shape=shapes,
        in_specs=[smem, smem, hbm, vmem, hbm, hbm, hbm, hbm],
        out_specs=(vmem,) * 3,
        scratch_shapes=[
            pltpu.VMEM(guide_table.shape, guide_table.dtype),
            pltpu.VMEM((count, width), half),
            pltpu.VMEM((width, depth), half),
            pltpu.VMEM((depth, width), half),
            pltpu.VMEM((units, 3, 1, width), jnp.float32),
            pltpu.VMEM((count, width), half),
            pltpu.VMEM((count, width), half),
            pltpu.VMEM((count, width), half),
            pltpu.VMEM((count, depth), half),
            pltpu.VMEM((2, width, count), half),
            pltpu.VMEM((2, count, width), half),
            pltpu.VMEM((count, width), jnp.float32),
            pltpu.VMEM((rows, width), jnp.float32),
            pltpu.VMEM((3, 8, width), jnp.float32),
            pltpu.VMEM((2, pieces, 2) + block, half),
            pltpu.VMEM((2, pieces) + block, half),
            pltpu.VMEM((pieces,) + near, half),
            pltpu.VMEM((pieces,) + near, half),
            pltpu.VMEM((2, far) + near, half),
            pltpu.VMEM((2, far) + near, half),
            pltpu.VMEM((pieces, 2) + deep, half),
            pltpu.VMEM((2, far, 2) + deep, half),
            pltpu.VMEM((2, far, 2) + deep, half),
            pltpu.VMEM((2,) + deep, half),
            pltpu.VMEM((2,) + deep, half),
            pltpu.VMEM((group, 8, 128), jnp.float32),
            pltpu.VMEM((group - 1, 8, 128), jnp.float32),
            dma((1,)), dma((2 + units,)), dma((hops,)), dma((hops,)), dma((2, pieces)), dma((2, pieces)),
            dma((pieces,)), dma((pieces,)), dma((2, far)), dma((2, far)), dma((2, far)),
            dma((2, far)), dma((2, far)), dma((2, far)), dma((2, far)), dma((2, far)),
            dma((2,)), dma((2,)), dma((group - 1,)), dma((group - 1,)),
        ],
        compiler_params=pltpu.CompilerParams(
            collective_id=0, has_side_effects=True, vmem_limit_bytes=62 * 1024 * 1024
        ),
    )(
        guide_bin.reshape(-1), time_step.reshape(-1), guide_table,
        section_table.transpose(1, 0, 2), inputs, out_grad,
        value_weight, proj_weight,
    )
    value_sum, proj_sum, table_sum = pl.pallas_call(
        place_kernel, out_shape=shapes, in_specs=[vmem] * 3, out_specs=(vmem,) * 3
    )(*sums)
    return (value_sum[None], proj_sum[None], table_sum.transpose(1, 0, 2))


def solution(mesh):
    return jax.shard_map(
        per_device,
        mesh=mesh,
        in_specs=(
            P(None, "dp", None),
            P(None, "dp", None),
            P(),
            P(),
            P(),
            P("section", None, None),
            P("section", None, None),
            P("section", None, None),
        ),
        out_specs=(P("section", "dp", None), P("section", "dp", None), P("section", None, "dp")),
        check_vma=False,
    )
```

```python
import functools
import math

import jax
import jax.numpy as jnp
from jax import lax
from jax.experimental import pallas as pl
from jax.experimental.pallas import tpu as pltpu
from jax.sharding import PartitionSpec as P

NORM_FLOOR = 0.1
PIECE_ROWS = 32
FORWARD_ROWS = 64
CHUNK_ROWS = 16
UNROLL = 2
TILE = 1536
OWN_DEEP = 2
TABLES_AHEAD = 1


def shifted(value, axis, steps):
    count = lax.axis_size(axis)
    leading, last = (max(0, -steps), min(count, count - steps))
    return lax.ppermute(value, axis, [(source, source + steps) for source in range(leading, last)])


def normalize(hidden):
    centre = jnp.mean(hidden, axis=-1, keepdims=True)
    centred = hidden - centre
    spread = jnp.mean(centred * centred, axis=-1, keepdims=True)
    inverse = lax.rsqrt(spread + NORM_FLOOR)
    return (centred * inverse, inverse)


def conditions(guide_bin, time_step, guide_table):
    total = guide_table.shape[1]
    half = total // 2
    frequency = jnp.exp(-math.log(10000.0) * jnp.arange(half, dtype=jnp.float32) / half)
    angle = time_step.astype(jnp.float32)[..., None] * frequency
    waves = jnp.concatenate([jnp.sin(angle), jnp.cos(angle)], axis=-1)
    bin_count = guide_table.shape[0]
    onehot = (guide_bin[..., None] == jnp.arange(bin_count, dtype=jnp.int32)).astype(jnp.float32)
    picked = jnp.einsum(
        "msb,bw->msw", onehot, guide_table.astype(jnp.float32), precision=lax.Precision.HIGHEST
    )
    return picked + 0.5 * waves


def contract_rows(left, right):
    return lax.dot_general(
        left, right, (((0,), (0,)), ((), ())), preferred_element_type=jnp.float32
    )


def forward_block(block_in, modulation, value_weight, proj_weight):
    width = block_in.shape[1]
    hidden = block_in.astype(jnp.float32)
    normed, inverse = normalize(hidden)
    shift = modulation[:, :width]
    scale = modulation[:, width : 2 * width]
    gate = modulation[:, 2 * width :]
    modulated = (normed * (1.0 + scale) + shift).astype(jnp.bfloat16)
    values = jnp.dot(modulated, value_weight, preferred_element_type=jnp.float32).astype(
        jnp.bfloat16
    )
    projected = jnp.dot(values, proj_weight, preferred_element_type=jnp.float32)
    block_out = (hidden + gate * projected).astype(jnp.bfloat16)
    return (block_out, modulated, values, projected)


def backward_block(block_in, projected, upstream, modulation, value_weight, proj_weight):
    width = block_in.shape[1]
    hidden = block_in.astype(jnp.float32)
    normed, inverse = normalize(hidden)
    scale = modulation[:, width : 2 * width]
    gate = modulation[:, 2 * width :]
    grad_up = upstream.astype(jnp.float32)
    grad_proj = (gate * grad_up).astype(jnp.bfloat16)
    grad_values = lax.dot_general(
        grad_proj, proj_weight, (((1,), (1,)), ((), ())), preferred_element_type=jnp.float32
    ).astype(jnp.bfloat16)
    grad_mod = lax.dot_general(
        grad_values, value_weight, (((1,), (1,)), ((), ())), preferred_element_type=jnp.float32
    )
    part_table = jnp.stack(
        [
            jnp.sum(grad_mod, axis=0),
            jnp.sum(grad_mod * normed, axis=0),
            jnp.sum(grad_up * projected, axis=0),
        ]
    )
    grad_norm = grad_mod * (1.0 + scale)
    centre_grad = jnp.mean(grad_norm, axis=-1, keepdims=True)
    cross = jnp.mean(grad_norm * normed, axis=-1, keepdims=True)
    grad_in = grad_up + inverse * (grad_norm - centre_grad - normed * cross)
    return (grad_in.astype(jnp.bfloat16), grad_values, grad_proj, part_table)


def per_device_scan(
    inputs, out_grad, guide_bin, time_step, guide_table, section_table, value_weight, proj_weight
):
    sections = lax.axis_size("section")
    section_id = lax.axis_index("section")
    position = lax.axis_index("dp")
    group_size = lax.axis_size("dp")
    tok_dev = inputs.shape[1]
    width = inputs.shape[2]
    value_width = value_weight.shape[2]
    batches = inputs.shape[0]
    samples = guide_bin.shape[1]
    tokens = tok_dev * group_size
    rows_per = tokens // samples
    parts = 1
    unit_rows = tok_dev // parts
    units = batches * parts
    condition = conditions(guide_bin, time_step, guide_table)
    weights_value = value_weight[0]
    weights_proj = proj_weight[0]
    section_row = section_table[0].reshape(-1)
    sample_ids = jnp.arange(samples, dtype=jnp.int32)

    def unit_modulation(unit_id):
        batch_id = unit_id // parts
        piece_id = unit_id % parts
        chosen = lax.dynamic_index_in_dim(condition, batch_id, 0, keepdims=False)
        global_rows = (
            position * tok_dev + piece_id * unit_rows + jnp.arange(unit_rows, dtype=jnp.int32)
        )
        owner = global_rows // rows_per
        onehot = (owner[:, None] == sample_ids[None, :]).astype(jnp.float32)
        picked = jnp.dot(
            onehot, chosen, precision=lax.Precision.HIGHEST, preferred_element_type=jnp.float32
        )
        return picked + section_row

    slots = units + 1
    keep_in = jnp.zeros((slots, unit_rows, width), jnp.bfloat16)
    keep_mod = jnp.zeros((slots, unit_rows, width), jnp.bfloat16)
    keep_val = jnp.zeros((slots, unit_rows, value_width), jnp.bfloat16)
    keep_proj = jnp.zeros((slots, unit_rows, width), jnp.float32)
    arriving = jnp.zeros((unit_rows, width), jnp.bfloat16)

    def forward_tick(carry, tick_id):
        incoming, saved_in, saved_mod, saved_val, saved_proj = carry
        unit_id = tick_id - section_id
        valid = (unit_id >= 0) & (unit_id < units)
        clipped = jnp.clip(unit_id, 0, units - 1)
        first = lax.dynamic_index_in_dim(inputs, clipped, 0, keepdims=False)
        block_in = jnp.where(section_id == 0, first, incoming)

        def forward_active(operand):
            return forward_block(operand, unit_modulation(clipped), weights_value, weights_proj)

        def forward_resting(operand):
            return (
                jnp.zeros_like(operand),
                jnp.zeros_like(operand),
                jnp.zeros((unit_rows, value_width), jnp.bfloat16),
                jnp.zeros((unit_rows, width), jnp.float32),
            )

        block_out, modulated, values, projected = lax.cond(
            valid, forward_active, forward_resting, block_in
        )
        slot_id = jnp.where(valid, unit_id, units)
        saved_in = lax.dynamic_update_index_in_dim(saved_in, block_in, slot_id, 0)
        saved_mod = lax.dynamic_update_index_in_dim(saved_mod, modulated, slot_id, 0)
        saved_val = lax.dynamic_update_index_in_dim(saved_val, values, slot_id, 0)
        saved_proj = lax.dynamic_update_index_in_dim(saved_proj, projected, slot_id, 0)
        sent = shifted(block_out, "section", 1)
        return ((sent, saved_in, saved_mod, saved_val, saved_proj), None)

    ticks = jnp.arange(units + sections - 1, dtype=jnp.int32)
    carry, unused = lax.scan(
        forward_tick, (arriving, keep_in, keep_mod, keep_val, keep_proj), ticks
    )
    arriving, keep_in, keep_mod, keep_val, keep_proj = carry
    store = jnp.zeros((slots, unit_rows, value_width), jnp.bfloat16)
    extra_zero = jnp.zeros((unit_rows, value_width), jnp.bfloat16)
    keep_grad = jnp.zeros((slots, unit_rows, width), jnp.bfloat16)
    proj_sum = jnp.zeros((value_width, width), jnp.float32)
    table_sum = jnp.zeros((3, width), jnp.float32)

    def backward_tick(carry, tick_id):
        incoming, store_now, grads_now, proj_now, table_now = carry
        unit_id = tick_id - (sections - 1 - section_id)
        valid = (unit_id >= 0) & (unit_id < units)
        clipped = jnp.clip(unit_id, 0, units - 1)
        last = lax.dynamic_index_in_dim(out_grad, clipped, 0, keepdims=False)
        upstream = jnp.where(section_id == sections - 1, last, incoming)
        block_in = lax.dynamic_index_in_dim(keep_in, clipped, 0, keepdims=False)
        modulated = lax.dynamic_index_in_dim(keep_mod, clipped, 0, keepdims=False)
        values = lax.dynamic_index_in_dim(keep_val, clipped, 0, keepdims=False)
        projected = lax.dynamic_index_in_dim(keep_proj, clipped, 0, keepdims=False)

        def backward_active(operand):
            grad_in, grad_values, grad_proj, part_table = backward_block(
                block_in, projected, operand, unit_modulation(clipped), weights_value, weights_proj
            )
            part_proj = jnp.zeros((value_width, width), jnp.float32)
            return (grad_in, grad_values, grad_proj, part_proj, part_table)

        def backward_resting(operand):
            return (
                jnp.zeros_like(operand),
                extra_zero,
                jnp.zeros((unit_rows, width), jnp.bfloat16),
                jnp.zeros((value_width, width), jnp.float32),
                jnp.zeros((3, width), jnp.float32),
            )

        grad_in, extra, grad_proj, part_proj, part_table = lax.cond(
            valid, backward_active, backward_resting, upstream
        )
        slot_id = jnp.where(valid, unit_id, units)
        store_now = lax.dynamic_update_index_in_dim(store_now, extra, slot_id, 0)
        grads_now = lax.dynamic_update_index_in_dim(grads_now, grad_proj, slot_id, 0)
        sent = shifted(grad_in, "section", -1)
        return ((sent, store_now, grads_now, proj_now + part_proj, table_now + part_table), None)

    carry, unused = lax.scan(
        backward_tick, (arriving, store, keep_grad, proj_sum, table_sum), ticks
    )
    arriving, store, keep_grad, proj_sum, table_sum = carry
    mod_rows = keep_mod[:units].reshape(units * unit_rows, width)
    grad_rows = store[:units].reshape(units * unit_rows, value_width)
    columns = mod_rows
    value_part = lax.psum_scatter(
        contract_rows(columns, grad_rows), "dp", scatter_dimension=0, tiled=True
    )
    val_rows = keep_val[:units].reshape(units * unit_rows, value_width)
    upper_rows = keep_grad[:units].reshape(units * unit_rows, width)
    columns = val_rows
    proj_part = lax.psum_scatter(
        contract_rows(columns, upper_rows), "dp", scatter_dimension=0, tiled=True
    )
    table_part = lax.psum_scatter(table_sum, "dp", scatter_dimension=1, tiled=True)
    return (value_part[None], proj_part[None], table_part[None])


MESH = pl.DeviceIdType.MESH


def step_kernel(far, bin_ref, time_ref, guide_hbm, section_ref, x_hbm, up_hbm, wv_hbm, wp_hbm,
                value_out, proj_out, table_out, guide_ref,
                local_s, wv_s, wp_s, rows_s, arrive_s, send_s, mod_s, val_s, left_s, right_s,
                wide_s, part_s, tab_s, made_s, core_in, side_out, side_in, low_in, high_in,
                deep_s, deep_low, deep_high, cross_out, cross_in,
                tables_s, tables_in, small_sem, load_sem, hop_send, hop_recv, core_send, core_recv,
                side_send, side_recv, low_send, low_recv, high_send, high_recv,
                down_send, down_recv, rise_send, rise_recv, cross_send, cross_recv,
                table_send, table_recv):
    units, unit_rows = x_hbm.shape[0], x_hbm.shape[1]
    count, width = local_s.shape
    depth = wv_s.shape[1]
    hops = hop_send.shape[0]
    piece = count // hops
    per_unit = unit_rows // piece
    group = 4 * far
    section = lax.axis_index("section")
    me = lax.axis_index("dp")
    core, side, place = me % 2, (me // 2) % 2, me // 4

    load_guide = pltpu.make_async_copy(guide_hbm, guide_ref, small_sem.at[0])
    load_guide.start()

    def load_rows(source, unit):
        part = pl.ds(unit * unit_rows, unit_rows)
        return pltpu.make_async_copy(source.at[unit], local_s.at[part], load_sem.at[2 + unit])

    load_value = pltpu.make_async_copy(wv_hbm.at[0], wv_s, load_sem.at[0])
    load_proj = pltpu.make_async_copy(wp_hbm.at[0], wp_s, load_sem.at[1])

    @pl.when(section == 0)
    def load_first():
        load_rows(x_hbm, 0).start()
        load_value.start()
        load_proj.start()
        for unit in range(1, units):
            load_rows(x_hbm, unit).start()

    @pl.when(section == 1)
    def load_last():
        load_rows(up_hbm, 0).start()
        load_proj.start()
        load_value.start()
        for unit in range(1, units):
            load_rows(up_hbm, unit).start()

    barrier = pltpu.get_barrier_semaphore()
    pl.semaphore_signal(
        barrier, inc=1, device_id={"section": 1 - section}, device_id_type=MESH
    )
    for step in range(1, group):
        pl.semaphore_signal(
            barrier, inc=1, device_id={"dp": (me + step) % group}, device_id_type=MESH
        )

    load_guide.wait()
    total = guide_ref.shape[1]
    half = total // 2
    samples = bin_ref.shape[0] // units
    sample = (me * unit_rows) // (unit_rows * group // samples)
    lane = lax.broadcasted_iota(jnp.int32, (units, half), 1).astype(jnp.float32)
    frequency = jnp.exp(-math.log(10000.0) * lane / half)
    which = lax.broadcasted_iota(jnp.int32, (units, half), 0)
    times = jnp.zeros((units, half), jnp.float32)
    for unit in range(units):
        time = time_ref[unit * samples + sample].astype(jnp.float32)
        times = jnp.where(which == unit, time, times)
    angle = times * frequency
    waves = jnp.concatenate([jnp.sin(angle), jnp.cos(angle)], axis=1)
    table = guide_ref[...].astype(jnp.float32)
    bins = lax.broadcasted_iota(jnp.int32, table.shape, 0)
    for unit in range(units):
        picked = jnp.sum(
            jnp.where(bins == bin_ref[unit * samples + sample], table, 0.0),
            axis=0, keepdims=True,
        )
        picked = picked + 0.5 * waves[unit:unit + 1]
        for index in range(3):
            lanes = slice(index * width, (index + 1) * width)
            rows_s[unit, index] = picked[:, lanes] + section_ref[index]
    tab_s[...] = jnp.zeros_like(tab_s)

    def hop(index):
        part = pl.ds(pl.multiple_of(index * piece, piece), piece)
        return pltpu.make_async_remote_copy(
            src_ref=send_s.at[part],
            dst_ref=arrive_s.at[part],
            send_sem=hop_send.at[index],
            recv_sem=hop_recv.at[index],
            device_id={"section": 1 - section},
            device_id_type=MESH,
        )

    def each_chunk(start, size, body):
        tall = math.gcd(size, CHUNK_ROWS)

        @pl.loop(0, size // tall, unroll=min(UNROLL, size // tall))
        def step(index):
            body(pl.ds(pl.multiple_of(start + index * tall, tall), tall), index * tall)

    def multiply(size, body):
        tile = math.gcd(size, TILE)

        @pl.loop(0, size // tile)
        def step(index):
            body(pl.ds(pl.multiple_of(index * tile, tile), tile))

    def add_rows(index, value):
        rows = value.shape[0]
        tab_s[index] += jnp.sum(value.reshape(rows // 8, 8, width), axis=0)

    def to_depth(rows, part):
        val_s[rows, part] = jnp.dot(
            mod_s[rows], wv_s[:, part], preferred_element_type=jnp.float32
        ).astype(jnp.bfloat16)

    def to_width(rows, part):
        return jnp.dot(val_s[rows], wp_s[:, part], preferred_element_type=jnp.float32)

    def to_values(rows):
        def body(part):
            right_s[1, rows, part] = lax.dot_general(
                right_s[0, rows], wp_s[part, :], (((1,), (1,)), ((), ())),
                preferred_element_type=jnp.float32,
            ).astype(jnp.bfloat16)

        multiply(depth, body)

    def to_mod(rows, target, target_rows):
        def body(part):
            target[target_rows, part] = lax.dot_general(
                right_s[1, rows], wv_s[part, :], (((1,), (1,)), ((), ())),
                preferred_element_type=jnp.float32,
            )

        multiply(width, body)

    def unit_rows_at(unit):
        return pl.ds(pl.multiple_of(unit * unit_rows, unit_rows), unit_rows)

    def turn_left(unit):
        part = unit_rows_at(unit)
        left_s[0, :, part] = val_s[part].T
        left_s[1, :, part] = mod_s[part].T

    def forward(index, size):
        start = pl.multiple_of(index * size, size)
        unit = start // unit_rows
        rows = pl.ds(start, size)

        def modulate(part, unused):
            normed, inverse = normalize(local_s[part].astype(jnp.float32))
            scaled = normed * (1.0 + rows_s[unit, 1]) + rows_s[unit, 0]
            mod_s[part] = scaled.astype(jnp.bfloat16)

        each_chunk(start, size, modulate)
        multiply(depth, lambda part: to_depth(rows, part))

        @pl.when(index == 0)
        def load_second():
            load_proj.wait()

        def second(part):
            wide_s[rows, part] = to_width(rows, part)

        multiply(width, second)

        @pl.when(index == 0)
        def enter():
            for unit in range(1, units):
                load_rows(x_hbm, unit).wait()
            pl.semaphore_wait(barrier, group)

        def add_gated(part, unused):
            hidden = local_s[part].astype(jnp.float32)
            block_out = hidden + rows_s[unit, 2] * wide_s[part]
            send_s[part] = block_out.astype(jnp.bfloat16)

        for at in range(size // piece):
            each_chunk(start + at * piece, piece, add_gated)
            hop(index * (size // piece) + at).start()

    def receive(index):
        start = pl.multiple_of(index * piece, piece)
        unit = start // unit_rows
        hop(index).wait_recv()

        def body(part, unused):
            grad_up = arrive_s[part].astype(jnp.float32)
            right_s[0, part] = (rows_s[unit, 2] * grad_up).astype(jnp.bfloat16)
            add_rows(2, grad_up * wide_s[part])

        each_chunk(start, piece, body)

    def table_rows(unit):
        to_mod(unit_rows_at(unit), part_s, slice(None))

        def body(part, offset):
            normed, inverse = normalize(local_s[part].astype(jnp.float32))
            grad_mod = part_s[pl.ds(offset, part.size)]
            add_rows(0, grad_mod)
            add_rows(1, grad_mod * normed)

        each_chunk(unit * unit_rows, unit_rows, body)

    @pl.when(section == 0)
    def earlier():
        load_rows(x_hbm, 0).wait()
        load_value.wait()
        size = math.gcd(unit_rows, FORWARD_ROWS)

        @pl.loop(0, units)
        def out(unit):
            @pl.loop(0, unit_rows // size)
            def some(at):
                forward(unit * (unit_rows // size) + at, size)

            turn_left(unit)

        @pl.loop(0, units)
        def back(unit):
            @pl.loop(0, per_unit)
            def one(at):
                receive(unit * per_unit + at)

            @pl.when(unit < units - 1)
            def values_now():
                to_values(unit_rows_at(unit))

            @pl.when(unit < min(TABLES_AHEAD, units - 1))
            def tables_now():
                table_rows(unit)

    def grads_ahead(unit):
        def body(part, unused):
            grad_up = local_s[part].astype(jnp.float32)
            right_s[0, part] = (rows_s[unit, 2] * grad_up).astype(jnp.bfloat16)

        each_chunk(unit * unit_rows, unit_rows, body)
        to_values(unit_rows_at(unit))

    def mods_ahead(unit):
        rows = unit_rows_at(unit)
        to_mod(rows, wide_s, rows)

    def values_behind(unit):
        multiply(depth, lambda part: to_depth(unit_rows_at(unit), part))

    def gates_behind(unit):
        rows = unit_rows_at(unit)

        def second(part):
            part_s[:, part] = to_width(rows, part)

        multiply(width, second)

        def body(part, offset):
            add_rows(2, local_s[part].astype(jnp.float32) * part_s[pl.ds(offset, part.size)])

        each_chunk(unit * unit_rows, unit_rows, body)

    def answer(index):
        start = pl.multiple_of(index * piece, piece)
        unit = start // unit_rows
        hop(index).wait_recv()

        def body(part, unused):
            normed, inverse = normalize(arrive_s[part].astype(jnp.float32))
            scale = 1.0 + rows_s[unit, 1]
            mod_s[part] = (normed * scale + rows_s[unit, 0]).astype(jnp.bfloat16)
            grad_mod = wide_s[part]
            add_rows(0, grad_mod)
            add_rows(1, grad_mod * normed)
            grad_norm = grad_mod * scale
            centre_grad = jnp.mean(grad_norm, axis=-1, keepdims=True)
            cross = jnp.mean(grad_norm * normed, axis=-1, keepdims=True)
            grad_up = local_s[part].astype(jnp.float32)
            grad_in = grad_up + inverse * (grad_norm - centre_grad - normed * cross)
            send_s[part] = grad_in.astype(jnp.bfloat16)

        each_chunk(start, piece, body)
        hop(index).start()

    @pl.when(section == 1)
    def later():
        load_rows(up_hbm, 0).wait()
        load_proj.wait()
        load_value.wait()
        for unit in range(1, units):
            load_rows(up_hbm, unit).wait()
        for unit in range(min(2, units)):
            grads_ahead(unit)
            mods_ahead(unit)
        pl.semaphore_wait(barrier, group)

        @pl.loop(0, units)
        def both(unit):
            @pl.loop(0, per_unit)
            def one(at):
                answer(unit * per_unit + at)

                @pl.when((at == 0) & (unit + 2 < units))
                def job_grads():
                    grads_ahead(unit + 2)

                @pl.when((at == 1) & (unit + 2 < units))
                def job_mods():
                    mods_ahead(unit + 2)

                @pl.when((at == 2 % per_unit) & (unit >= 1))
                def job_values():
                    values_behind(unit - 1)

        values_behind(units - 1)

        @pl.loop(0, units)
        def turn(unit):
            turn_left(unit)

    ranks = [sorted(range(far), key=lambda block: -abs(block - spot)) for spot in range(far)]
    order = [(matrix, rank) for rank in range(far - 1) for matrix in range(2)]
    order = order + [(0, far - 1), (1, far - 1)]
    pieces = len(order)
    block_rows = left_s.shape[1] // group
    per_matrix = far - 1

    def chosen(values):
        result = 0
        for spot in range(far):
            away = (place - spot + far) % far
            result = result + values[spot] * (1 - (away + far - 1) // far)
        return result

    blocks = [chosen([ranks[spot][rank] for spot in range(far)]) for rank in range(far)]

    def partial(turn, index):
        matrix, rank = order[index]
        which = (1 - side) if turn == 0 else side
        first = pl.multiple_of((blocks[rank] * 2 + which) * 2 * block_rows, 2 * block_rows)
        product = jnp.dot(
            left_s[matrix, pl.ds(first, 2 * block_rows)], right_s[matrix],
            preferred_element_type=jnp.float32,
        )
        made_s[turn, index] = product.astype(jnp.bfloat16).reshape(2, block_rows, width)

    def core_copy(turn, index):
        return pltpu.make_async_remote_copy(
            src_ref=made_s.at[turn, index, 1 - core],
            dst_ref=core_in.at[turn, index],
            send_sem=core_send.at[turn, index],
            recv_sem=core_recv.at[turn, index],
            device_id={"dp": me + 1 - 2 * core},
            device_id_type=MESH,
        )

    def side_copy(index):
        return pltpu.make_async_remote_copy(
            src_ref=side_out.at[index],
            dst_ref=side_in.at[index],
            send_sem=side_send.at[index],
            recv_sem=side_recv.at[index],
            device_id={"dp": me + 2 - 4 * side},
            device_id_type=MESH,
        )

    def over_block(body):
        tall = math.gcd(block_rows, 16)

        @pl.loop(0, block_rows // tall)
        def step(at):
            body(pl.ds(pl.multiple_of(at * tall, tall), tall))

    near = side_out.shape[2]
    near_lanes, deep_lanes = slice(0, near), slice(near, width)
    spot_now = [0]

    def rank_of(block):
        return ranks[spot_now[0]].index(block)

    def row_copy(source, target, send_sem, recv_sem, matrix, block, away):
        return pltpu.make_async_remote_copy(
            src_ref=source.at[order.index((matrix, rank_of(block)))],
            dst_ref=target.at[matrix, block],
            send_sem=send_sem.at[matrix, block],
            recv_sem=recv_sem.at[matrix, block],
            device_id={"dp": (me + group + 4 * away) % group},
            device_id_type=MESH,
        )

    def up_copy(matrix, block):
        return row_copy(side_out, low_in, low_send, low_recv, matrix, block, 1)

    def down_copy(matrix, block):
        return row_copy(side_out, high_in, high_send, high_recv, matrix, block, -1)

    def deep_up(matrix, block):
        return row_copy(deep_s, deep_low, rise_send, rise_recv, matrix, block, 1)

    def deep_down(matrix, block):
        return row_copy(deep_s, deep_high, down_send, down_recv, matrix, block, -1)

    def cross_copy(matrix):
        return pltpu.make_async_remote_copy(
            src_ref=cross_out.at[matrix],
            dst_ref=cross_in.at[matrix],
            send_sem=cross_send.at[matrix],
            recv_sem=cross_recv.at[matrix],
            device_id={"dp": me + 2 - 4 * side},
            device_id_type=MESH,
        )

    outs = (proj_out, value_out)

    def core_sum(turn, index, part, lanes):
        mine = made_s[turn, index, core, part, lanes].astype(jnp.float32)
        return mine + core_in[turn, index, part, lanes].astype(jnp.float32)

    def send_side(index):
        core_copy(0, index).wait_recv()

        def add(part):
            side_out[index, part] = core_sum(0, index, part, near_lanes).astype(jnp.bfloat16)
            deep_s[index, 0, part] = core_sum(0, index, part, deep_lanes).astype(jnp.bfloat16)

        over_block(add)
        side_copy(index).start()
        core_copy(1, index).wait_recv()

        def add_own(part):
            deep_s[index, 1, part] = core_sum(1, index, part, deep_lanes).astype(jnp.bfloat16)

        over_block(add_own)

    def terms_of(spot, matrix, block, up, down, low, high):
        terms = []
        if block >= spot and spot > 0:
            up(matrix, block).wait_recv()
            terms.append(low)
        if block <= spot and spot < far - 1:
            down(matrix, block).wait_recv()
            terms.append(high)
        return terms

    def deep_chain(spot, index):
        spot_now[0] = spot
        matrix, rank = order[index]
        block = ranks[spot][rank]
        terms = terms_of(spot, matrix, block, deep_up, deep_down, deep_low, deep_high)

        def add(part):
            for which in range(2):
                mine = deep_s[index, which, part].astype(jnp.float32)
                for term in terms:
                    mine = mine + term[matrix, block, which, part].astype(jnp.float32)
                if block != spot:
                    deep_s[index, which, part] = mine.astype(jnp.bfloat16)
                elif which == 0:
                    cross_out[matrix, part] = mine.astype(jnp.bfloat16)
                else:
                    outs[matrix][part, deep_lanes] = mine

        if terms or block == spot:
            over_block(add)
        if block > spot:
            deep_up(matrix, block).start()
        elif block < spot:
            deep_down(matrix, block).start()
        else:
            cross_copy(matrix).start()

    def chain(spot, index):
        spot_now[0] = spot
        matrix, rank = order[index]
        block = ranks[spot][rank]
        side_copy(index).wait_send()
        side_copy(index).wait_recv()
        terms = terms_of(spot, matrix, block, up_copy, down_copy, low_in, high_in)

        def add(part):
            mine = core_sum(1, index, part, near_lanes)
            mine = mine + side_in[index, part].astype(jnp.float32)
            for term in terms:
                mine = mine + term[matrix, block, part].astype(jnp.float32)
            if block == spot:
                outs[matrix][part, near_lanes] = mine
            else:
                side_out[index, part] = mine.astype(jnp.bfloat16)

        over_block(add)
        if block > spot:
            up_copy(matrix, block).start()
        elif block < spot:
            down_copy(matrix, block).start()

    def at_spots(spots, body):
        for spot in spots:
            @pl.when(place == spot)
            def run(spot=spot):
                body(spot)

    ends = sorted({0, far - 1})

    def early(index):
        send_side(index)
        if order[index][1] < far - 1:
            at_spots(ends, lambda spot: deep_chain(spot, index))

    for index in range(pieces):
        if index == 1:
            @pl.when(section == 0)
            def values_last():
                to_values(unit_rows_at(units - 1))

        for turn in range(2):
            partial(turn, index)
            core_copy(turn, index).start()
        if index > 0:
            early(index - 1)
    early(pieces - 1)

    def pass_deep(spot):
        for index in range(pieces):
            if order[index][1] < far - 1:
                deep_chain(spot, index)

    def own_deep(spot):
        for index in range(pieces):
            if order[index][1] == far - 1:
                deep_chain(spot, index)

    at_spots([spot for spot in range(far) if spot not in ends], pass_deep)

    def finish(spot):
        spot_now[0] = spot
        for matrix in range(2):
            for block in range(far):
                if block > spot:
                    up_copy(matrix, block).wait_send()
                    deep_up(matrix, block).wait_send()
                elif block < spot:
                    down_copy(matrix, block).wait_send()
                    deep_down(matrix, block).wait_send()

    def stage(indices):
        def body(spot):
            for index in indices:
                chain(spot, index)

        at_spots(range(far), body)

    ahead = min(units, pieces - 1)
    for index in range(ahead):
        stage([index])
        if index == min(OWN_DEEP, ahead - 1):
            at_spots(range(far), own_deep)

        last = index == ahead - 1
        behind = (index + TABLES_AHEAD) % units
        spare = [behind] if ahead == units else range(index, units if last else index + 1)

        @pl.when(section == 0)
        def tables(spare=spare):
            for unit in spare:
                if unit >= min(TABLES_AHEAD, units - 1):
                    table_rows(unit)

        @pl.when(section == 1)
        def gates(index=index):
            for unit in range(index, units if last else index + 1):
                gates_behind(unit)

    lanes = table_out.shape[2]
    table = jnp.concatenate(
        [jnp.sum(tab_s[index], axis=0, keepdims=True) for index in range(3)]
        + [jnp.zeros((5, width), jnp.float32)], axis=0,
    )
    for owner in range(group):
        tables_s[owner, :, :lanes] = table[:, owner * lanes:(owner + 1) * lanes]

    def table_copy(step):
        return pltpu.make_async_remote_copy(
            src_ref=tables_s.at[(me + step) % group],
            dst_ref=tables_in.at[step - 1],
            send_sem=table_send.at[step - 1],
            recv_sem=table_recv.at[step - 1],
            device_id={"dp": (me + step) % group},
            device_id_type=MESH,
        )

    for step in range(1, group):
        table_copy(step).start()
    stage(range(ahead, pieces - 2))
    sums = tables_s[me]
    for step in range(1, group):
        table_copy(step).wait_recv()
        sums = sums + tables_in[step - 1]
    for row in range(3):
        table_out[row] = sums[row:row + 1, :lanes]
    stage(range(max(ahead, pieces - 2), pieces))
    for matrix in range(2):
        cross_copy(matrix).wait_recv()

        def add_cross(part):
            outs[matrix][part, deep_lanes] += cross_in[matrix, part].astype(jnp.float32)

        over_block(add_cross)

    @pl.loop(0, hops)
    def sent(index):
        hop(index).wait_send()

    for index in range(pieces):
        core_copy(0, index).wait_send()
        core_copy(1, index).wait_send()
    for matrix in range(2):
        cross_copy(matrix).wait_send()
    for step in range(1, group):
        table_copy(step).wait_send()
    at_spots(range(far), finish)


def place_kernel(value_ref, proj_ref, table_ref, value_out, proj_out, table_out):
    value_out[...] = value_ref[...]
    proj_out[...] = proj_ref[...]
    table_out[...] = table_ref[...]


def per_device(
    inputs, out_grad, guide_bin, time_step, guide_table, section_table, value_weight, proj_weight
):
    units, rows, width = inputs.shape
    depth = value_weight.shape[2]
    group = lax.axis_size("dp")
    per_sample = rows * group // guide_bin.shape[1]
    if (lax.axis_size("section") != 2 or group % 4 or per_sample % rows or rows % 128
            or width != depth or width % (group * 16) or width < 768):
        return per_device_scan(
            inputs, out_grad, guide_bin, time_step, guide_table, section_table,
            value_weight, proj_weight,
        )
    far = group // 4
    count = units * rows
    piece = math.gcd(rows, PIECE_ROWS)
    hops = count // piece
    block = (width // group, width)
    pieces = 2 * far
    deep = (block[0], width // 6 // 128 * 128)
    near = (block[0], width - deep[1])
    lanes = width // group
    vmem = pl.BlockSpec(memory_space=pltpu.VMEM)
    smem = pl.BlockSpec(memory_space=pltpu.SMEM)
    hbm = pl.BlockSpec(memory_space=pl.ANY)
    dma = pltpu.SemaphoreType.DMA
    half = jnp.bfloat16
    shapes = (
        jax.ShapeDtypeStruct(block, jnp.float32),
        jax.ShapeDtypeStruct(block, jnp.float32),
        jax.ShapeDtypeStruct((3, 1, lanes), jnp.float32),
    )
    sums = pl.pallas_call(
        functools.partial(step_kernel, far),
        out_shape=shapes,
        in_specs=[smem, smem, hbm, vmem, hbm, hbm, hbm, hbm],
        out_specs=(vmem,) * 3,
        scratch_shapes=[
            pltpu.VMEM(guide_table.shape, guide_table.dtype),
            pltpu.VMEM((count, width), half),
            pltpu.VMEM((width, depth), half),
            pltpu.VMEM((depth, width), half),
            pltpu.VMEM((units, 3, 1, width), jnp.float32),
            pltpu.VMEM((count, width), half),
            pltpu.VMEM((count, width), half),
            pltpu.VMEM((count, width), half),
            pltpu.VMEM((count, depth), half),
            pltpu.VMEM((2, width, count), half),
            pltpu.VMEM((2, count, width), half),
            pltpu.VMEM((count, width), jnp.float32),
            pltpu.VMEM((rows, width), jnp.float32),
            pltpu.VMEM((3, 8, width), jnp.float32),
            pltpu.VMEM((2, pieces, 2) + block, half),
            pltpu.VMEM((2, pieces) + block, half),
            pltpu.VMEM((pieces,) + near, half),
            pltpu.VMEM((pieces,) + near, half),
            pltpu.VMEM((2, far) + near, half),
            pltpu.VMEM((2, far) + near, half),
            pltpu.VMEM((pieces, 2) + deep, half),
            pltpu.VMEM((2, far, 2) + deep, half),
            pltpu.VMEM((2, far, 2) + deep, half),
            pltpu.VMEM((2,) + deep, half),
            pltpu.VMEM((2,) + deep, half),
            pltpu.VMEM((group, 8, 128), jnp.float32),
            pltpu.VMEM((group - 1, 8, 128), jnp.float32),
            dma((1,)), dma((2 + units,)), dma((hops,)), dma((hops,)), dma((2, pieces)), dma((2, pieces)),
            dma((pieces,)), dma((pieces,)), dma((2, far)), dma((2, far)), dma((2, far)),
            dma((2, far)), dma((2, far)), dma((2, far)), dma((2, far)), dma((2, far)),
            dma((2,)), dma((2,)), dma((group - 1,)), dma((group - 1,)),
        ],
        compiler_params=pltpu.CompilerParams(
            collective_id=0, has_side_effects=True, vmem_limit_bytes=62 * 1024 * 1024
        ),
    )(
        guide_bin.reshape(-1), time_step.reshape(-1), guide_table,
        section_table.transpose(1, 0, 2), inputs, out_grad,
        value_weight, proj_weight,
    )
    value_sum, proj_sum, table_sum = pl.pallas_call(
        place_kernel, out_shape=shapes, in_specs=[vmem] * 3, out_specs=(vmem,) * 3
    )(*sums)
    return (value_sum[None], proj_sum[None], table_sum.transpose(1, 0, 2))


def solution(mesh):
    return jax.shard_map(
        per_device,
        mesh=mesh,
        in_specs=(
            P(None, "dp", None),
            P(None, "dp", None),
            P(),
            P(),
            P(),
            P("section", None, None),
            P("section", None, None),
            P("section", None, None),
        ),
        out_specs=(P("section", "dp", None), P("section", "dp", None), P("section", None, "dp")),
        check_vma=False,
    )
```
